32 devices in a mesh: rows: 8 (over y, x, core), cols: 4 (over z).
Axes of the slice: x: 2, y: 2, z: 4, core: 2. Of those that a mesh axis runs over, the one named last changes fastest.
Arguments:
- block_values: bfloat16 [16384, 128], P(('rows', 'cols')), may hold values from -6 to 6
- block_length: int32 [16384], P(('rows', 'cols')), may hold values from 1 to 128
- block_owner: int32 [16384], P(('rows', 'cols')), may hold values from 0 to 4095, as said below
- block_second: int32 [16384], P(('rows', 'cols')), may hold values from 0 to 4095, as said below
- block_third: int32 [16384, 128], P(('rows', 'cols')), may hold values from 0 to 8191
- live_blocks: int32 [32], P(('rows', 'cols')), may hold values from 1 to 512, as said below
- second_factor: bfloat16 [4096, 256], P('cols', 'rows')
- third_factor: bfloat16 [8192, 256], P('cols', 'rows'), may hold values from -6 to 6
Outputs:
- first_factor: float32 [4096, 256], P('cols', 'rows')
The draws below stay inside these ranges and needn't reach their ends.
Inputs may be any that keep to these rules, and one draw needn't show every extreme that they name: `block_owner`: slot b lies on device d = b // 512 with index r along rows; its row lies in r * 4096 // 8 up to (r + 1) * 4096 // 8 - 1, the device's mode-1 slab. `block_second`: slot b lies on device d = b // 512 with index c along cols; its row lies in c * 4096 // 4 up to (c + 1) * 4096 // 4 - 1. `live_blocks`: some device uses all 512 slots in every draw.
All inputs are finite; a program needn't handle non-finite values.
Results may differ from the reference program's by a relative error of at most 0.0003.
Values may be sent and summed in bfloat16 or wider, within the bound.
A program may use at most 128 MiB of HBM per device.

```python
import jax
import jax.numpy as jnp
from jax import lax

R = 256
L = 128
NB_DEV = 512
BLOCKS = 16384
I = 4096
J = 4096
K = 8192
N_ROWS = 8
N_COLS = 4
DEVICES = 32


def draw_block_owner(key, part):
    slot = jnp.arange(NB_DEV * DEVICES, dtype=jnp.int32)
    device = slot // NB_DEV
    slab = I // N_ROWS
    offset = jax.random.randint(key, (NB_DEV * DEVICES,), 0, slab, dtype=jnp.int32)
    return device // N_COLS * slab + offset


def draw_block_second(key, part):
    slot = jnp.arange(NB_DEV * DEVICES, dtype=jnp.int32)
    device = slot // NB_DEV
    span = J // N_COLS
    offset = jax.random.randint(jax.random.fold_in(key, 7), (NB_DEV * DEVICES,), 0, span, dtype=jnp.int32)
    return device % N_COLS * span + offset


def draw_live_blocks(key, part):
    first, second = jax.random.split(jax.random.fold_in(key, 11))
    counts = jax.random.randint(first, (DEVICES,), 1, NB_DEV + 1, dtype=jnp.int32)
    full = jax.random.randint(second, (), 0, DEVICES, dtype=jnp.int32)
    return jnp.where(jnp.arange(DEVICES, dtype=jnp.int32) == full, NB_DEV, counts)


def draw_second_factor(key, part):
    first = jax.random.fold_in(jax.random.fold_in(key, 13), 0)
    third = jax.random.fold_in(jax.random.fold_in(key, 13), 2)
    trend = 3.0 ** (jnp.arange(J, dtype=jnp.float32) / J)
    scale = trend * 10.0 ** jax.random.uniform(first, (J,), jnp.float32)
    base = jax.random.normal(third, (J, R), jnp.float32)
    return (scale[:, None] * base).astype(jnp.bfloat16)


def place_ends(drawn, stream_key, low, top_value):
    longest = drawn.shape.index(max(drawn.shape))
    spots = []
    for shift in (0, 1):
        where = [jax.random.randint(jax.random.fold_in(stream_key, axis), (), 0, length) for axis, length in enumerate(drawn.shape)]
        where[longest] = (where[longest] + shift) % drawn.shape[longest]
        spots.append(tuple(where))
    return drawn.at[spots[0]].set(low).at[spots[1]].set(top_value)


def steps_of(key, dims, cuts, smallest, high):
    gain = 1.0
    for dim, blocks in cuts:
        draws = jax.random.uniform(jax.random.fold_in(jax.random.fold_in(key, 6), dim), (blocks,), jnp.float32, smallest / len(cuts), high / len(cuts))
        gain = gain * jnp.repeat(jnp.exp(draws), dims[dim] // blocks).reshape((-1,) + (1,) * (len(dims) - 1 - dim))
    return gain


def scatter_about(own_key, dims, deviation, reach, shards=(), kind=jnp.bfloat16):
    values = jax.random.normal(own_key, dims, jnp.float32) * deviation
    if len(shards) > 0:
        values = steps_of(own_key, dims, shards, -0.22, 0.18) * values
    return jnp.clip(values, min=-reach, max=reach).astype(kind)


def setup_inputs(seed: int = 0) -> dict:
    key_of = jax.random.split(jax.random.key(seed), 9)
    return {
        "block_values": scatter_about(key_of[0], (BLOCKS, L), 1.0, 6.0, ((0, 32),)),
        "block_length": place_ends(jax.random.randint(key_of[1], (BLOCKS,), 1, L + 1), jax.random.fold_in(key_of[1], 1), 1, L).astype(jnp.int32),
        "block_owner": draw_block_owner(jax.random.fold_in(key_of[8], 71), 0),
        "block_second": draw_block_second(jax.random.fold_in(key_of[8], 71), 0),
        "block_third": place_ends(jax.random.randint(key_of[4], (BLOCKS, L), 0, K), jax.random.fold_in(key_of[4], 1), 0, K - 1).astype(jnp.int32),
        "live_blocks": draw_live_blocks(jax.random.fold_in(key_of[8], 71), 0),
        "second_factor": draw_second_factor(jax.random.fold_in(key_of[8], 71), 0),
        "third_factor": scatter_about(key_of[7], (K, R), 1.0, 6.0, ((0, 4), (1, 8))),
    }


def reference(block_values, block_length, block_owner, block_second, block_third, live_blocks, second_factor, third_factor):
    nblk = block_values.shape[0]
    width = block_values.shape[1]
    group = min(nblk, 512)
    position = jnp.arange(nblk, dtype=jnp.int32)
    live_block = position % NB_DEV < live_blocks[position // NB_DEV]
    lane = jnp.arange(width, dtype=jnp.int32)
    live = (lane[None, :] < block_length[:, None]) & live_block[:, None]
    masked = jnp.where(live, block_values, jnp.zeros((), jnp.bfloat16))
    steps = nblk // group

    def accumulate(total, pieces):
        values, third, second, owner = pieces
        rows = third_factor[third].astype(jnp.float32)
        fold = jnp.einsum('gt,gtr->gr', values.astype(jnp.float32), rows)
        contrib = second_factor[second].astype(jnp.float32) * fold
        return (total.at[owner].add(contrib), None)
    pieces = (masked.reshape(steps, group, width), block_third.reshape(steps, group, width), block_second.reshape(steps, group), block_owner.reshape(steps, group))
    start = jnp.zeros((I, R), jnp.float32)
    mttkrp, unused = lax.scan(accumulate, start, pieces)
    contract = (((0,), (0,)), ((), ()))
    gram_second = lax.dot_general(second_factor.astype(jnp.float32), second_factor.astype(jnp.float32), contract, preferred_element_type=jnp.float32) / J
    gram_third = lax.dot_general(third_factor.astype(jnp.float32), third_factor.astype(jnp.float32), contract, preferred_element_type=jnp.float32) / K
    gram = gram_second * gram_third
    factor = jnp.linalg.cholesky(gram)
    return jax.scipy.linalg.cho_solve((factor, True), mttkrp.T).T
```

```python
import functools

import jax
import jax.numpy as jnp
from jax import lax
from jax.experimental import pallas as pl
from jax.experimental.pallas import tpu as pltpu
from jax.sharding import PartitionSpec as P

LO = 128
TILE = 256
CHUNK = 32
BF = jnp.bfloat16
F32 = jnp.float32
NT = (((1,), (1,)), ((), ()))
NN = (((1,), (0,)), ((), ()))
EXACT = lax.Precision.HIGHEST
MESH = pl.DeviceIdType.MESH


def dot(a, b, dims, precision=None):
    return lax.dot_general(a, b, dims, precision=precision, preferred_element_type=F32)


def flipped(row, flip):
    target = row
    bit = 1
    while bit <= flip:
        if flip & bit:
            target = target + bit - 2 * bit * lax.rem(row // bit, 2)
        bit *= 2
    return target


class Gather:
    def __init__(self, n_rows, n_cols, both_ref, buf, sems):
        self.n_rows, self.n_cols, self.both, self.buf = n_rows, n_cols, both_ref, buf
        self.send_z, self.land_z, self.send_f, self.land_f, self.hand, self.take = sems
        self.rank = both_ref.shape[0]
        self.row, self.col = lax.axis_index("rows"), lax.axis_index("cols")
        self.partner = self.row + 1 - 2 * lax.rem(self.row, 2)
        self.bits = [b for b in (2**i for i in range(1, 16)) if b < n_rows]
        self.multi = [f for f in range(2, n_rows, 2) if f not in self.bits]
        orders = []
        for c in range(n_cols):
            others = [(abs(a - c), a - c) for a in range(n_cols)]
            orders.append([d for _, d in sorted(others)])
        self.delta = [sum((self.col == c).astype(jnp.int32) * orders[c][j] for c in range(n_cols)) for j in range(n_cols)]
        self.slot = [lax.rem(d + n_cols, n_cols) for d in self.delta]

    def area(self, block, slot, half=None):
        if half is None:
            return self.buf.at[slot, pl.ds(block * self.rank, self.rank), :]
        size = self.rank // 2
        return self.buf.at[slot, pl.ds(block * self.rank + half * size, size), :]

    def source(self, block, j, half=None):
        if block == 0 and j == 0:
            return self.both
        return self.area(block, self.slot[j], half)

    def z_copy(self, j, up):
        step = 1 if up else -1
        there = lax.rem(self.slot[j] - step + self.n_cols, self.n_cols)
        target = lax.rem(self.col + step + self.n_cols, self.n_cols)
        return pltpu.make_async_remote_copy(
            src_ref=self.source(0, j),
            dst_ref=self.area(0, there),
            send_sem=self.send_z.at[int(up), j],
            recv_sem=self.land_z.at[there],
            device_id=(self.row, target),
            device_id_type=MESH,
        )

    def z_moves(self, j):
        yield True, (self.delta[j] <= 0) & (self.col + 1 < self.n_cols)
        yield False, (self.delta[j] >= 0) & (self.col >= 1)

    def flip_copy(self, bit, block, j, half):
        there = block ^ bit
        part = None if there in self.bits else half
        return pltpu.make_async_remote_copy(
            src_ref=self.source(block, j, part),
            dst_ref=self.area(there, self.slot[j], part),
            send_sem=self.send_f.at[there // 2, j, half],
            recv_sem=self.land_f.at[there // 2, self.slot[j], half],
            device_id=(flipped(self.row, bit), self.col),
            device_id_type=MESH,
        )

    def route(self, flip, half):
        bits = [b for b in self.bits if flip & b]
        return bits[0] if half == 0 else bits[-1]

    def core_copy(self, block, j):
        return pltpu.make_async_remote_copy(
            src_ref=self.source(block, j),
            dst_ref=self.area(block + 1, self.slot[j]),
            send_sem=self.hand.at[block // 2, j],
            recv_sem=self.take.at[block // 2, self.slot[j]],
            device_id=(self.partner, self.col),
            device_id_type=MESH,
        )

    def begin(self):
        barrier = pltpu.get_barrier_semaphore()
        n = self.n_cols
        near = [(self.partner, self.col), (self.row, lax.rem(self.col + 1, n)), (self.row, lax.rem(self.col + n - 1, n))]
        near += [(flipped(self.row, b), self.col) for b in self.bits]
        for target in near:
            pl.semaphore_signal(barrier, inc=1, device_id=target, device_id_type=MESH)
        pl.semaphore_wait(barrier, len(near))
        self.own(0)

    def own(self, j):
        for up, there in self.z_moves(j):
            pl.when(there)(self.z_copy(j, up).start)
        for bit in self.bits:
            self.flip_copy(bit, 0, j, 0).start()
        self.core_copy(0, j).start()

    def relay_z(self, j):
        pltpu.make_async_copy(self.both, self.area(0, self.slot[j]), self.land_z.at[self.slot[j]]).wait()
        self.own(j)

    def relay_single(self, j):
        for block in self.bits:
            self.flip_copy(block, 0, j, 0).wait_recv()
            for flip in self.multi:
                for half in range(2):
                    bit = self.route(flip, half)
                    if flip ^ bit == block:
                        self.flip_copy(bit, block, j, half).start()
            self.core_copy(block, j).start()

    def relay_multi(self, j):
        for block in self.multi:
            for half in range(2):
                bit = self.route(block, half)
                self.flip_copy(bit, block ^ bit, j, half).wait_recv()
                for flip in self.multi:
                    bit = self.route(flip, half)
                    if flip ^ bit == block:
                        self.flip_copy(bit, block, j, half).start()
            self.core_copy(block, j).start()

    def arrived(self, j):
        for block in range(0, self.n_rows, 2):
            self.core_copy(block, j).wait_recv()

    def end(self):
        for j in range(self.n_cols):
            for up, there in self.z_moves(j):
                pl.when(there)(self.z_copy(j, up).wait_send)
            for bit in self.bits:
                self.flip_copy(bit, 0, j, 0).wait_send()
            for block in range(0, self.n_rows, 2):
                self.core_copy(block, j).wait_send()
                if block in self.multi:
                    for half in range(2):
                        bit = self.route(block, half)
                        self.flip_copy(bit, block ^ bit, j, half).wait_send()


def fold_kernel(n_rows, n_cols, third_rows, batch, *refs):
    count_ref, values_ref, length_ref, third_ref, second_ref, owner_ref, both_ref = refs[:7]
    out_ref, gram_second_ref, gram_ref, buf, dense, masked, index, fold, lengths = refs[7:16]
    gather = Gather(n_rows, n_cols, both_ref, buf, refs[16:])
    nblk, width = values_ref.shape
    rank, span = both_ref.shape
    n_hi = n_cols * third_rows // LO
    part_hi = third_rows // LO
    range_rows = span - third_rows
    row, col = lax.axis_index("rows"), lax.axis_index("cols")
    batches = nblk // batch
    gather.begin()

    buf[0, 0:rank, :] = both_ref[...]
    gram_ref[...] = jnp.zeros_like(gram_ref)
    gram_second_ref[...] = jnp.zeros_like(gram_second_ref)
    out_ref[...] = jnp.zeros_like(out_ref)
    for i in range(nblk // 128):
        line = length_ref[:, i * 128 : (i + 1) * 128]
        lengths[i * 128 : (i + 1) * 128, :] = jnp.broadcast_to(line, (128, 128)).T
    lane = lax.broadcasted_iota(jnp.int32, (nblk, width), 1)
    at_slot = lax.broadcasted_iota(jnp.int32, (nblk, width), 0)
    live = (lane < lengths[...]) & (at_slot < count_ref[0])
    masked[...] = jnp.where(live, values_ref[...].astype(F32), 0.0)
    turned = third_ref[...] - col * third_rows
    index[...] = jnp.where(turned < 0, turned + n_cols * third_rows, turned)

    at = lax.broadcasted_iota(jnp.int32, (max(LO, n_hi), width), 0).astype(F32).astype(BF)
    one = jnp.ones((16, width), BF)
    zero = jnp.zeros((16, width), BF)

    def spread(start, first):
        place = index[pl.ds(start, 8), :]
        value = masked[pl.ds(start, 8), :]
        high = lax.shift_right_logical(place, 7).astype(F32)
        low = (place & (LO - 1)).astype(F32)
        for j in range(8):
            high16 = jnp.broadcast_to(high[j : j + 1, :], (16, width)).astype(BF)
            low16 = jnp.broadcast_to(low[j : j + 1, :], (16, width)).astype(BF)
            value16 = jnp.broadcast_to(value[j : j + 1, :], (16, width)).astype(BF)
            left = [jnp.where(at[k : k + 16] == high16, value16, zero) for k in range(0, n_hi, 16)]
            right = [jnp.where(at[k : k + 16] == low16, one, zero) for k in range(0, LO, 16)]
            tile = dot(jnp.concatenate(left, axis=0), jnp.concatenate(right, axis=0), NT)
            dense[:, pl.ds(first + j, 1), :] = tile.reshape(n_hi, 1, LO)

    def fold_slot(j):
        slot = gather.slot[j]
        per = 4

        def tiles(i, carry):
            total = fold[...]
            for k in range(per):
                at_hi = slot * part_hi + (i * per + k) * (TILE // LO)
                x = jnp.concatenate([dense[at_hi + h, 0:batch, :] for h in range(TILE // LO)], axis=1)
                high = x.astype(BF)
                low = (x - high.astype(F32)).astype(BF)
                start = pl.multiple_of((i * per + k) * TILE, TILE)
                piece = buf[slot, :, pl.ds(start, TILE)]
                total = total + (dot(high, piece, NT) + dot(low, piece, NT))
            fold[...] = total
            return carry

        lax.fori_loop(0, third_rows // TILE // per, tiles, 0)

    def gram_slot(j):
        piece = buf[gather.slot[j], :, 0:third_rows]
        gram_ref[...] += dot(piece, piece, NT)
        piece = buf[gather.slot[j], :, third_rows:span]
        gram_second_ref[...] += dot(piece, piece, NT)

    def scatter(part):
        columns = slice(part * batch, (part + 1) * batch)
        second = buf[0, :, third_rows:span]
        at_second = lax.broadcasted_iota(jnp.int32, (range_rows, batch), 0) + col * range_rows
        pick = jnp.where(at_second == second_ref[:, columns], 1.0, 0.0).astype(BF)
        contrib = dot(second, pick, NN) * fold[...].T
        slab = out_ref.shape[1]
        at_owner = lax.broadcasted_iota(jnp.int32, (slab, batch), 0) + row * slab
        place = jnp.where(at_owner == owner_ref[:, columns], 1.0, 0.0).astype(BF)
        high = contrib.astype(BF)
        rest = contrib - high.astype(F32)
        middle = rest.astype(BF)
        low = (rest - middle.astype(F32)).astype(BF)
        out_ref[...] += dot(high, place, NT) + (dot(middle, place, NT) + dot(low, place, NT))

    steps = batch // CHUNK
    early = {}
    late = {}
    plan = [(0.25, gather.relay_z, 1), (0.25, gather.relay_single, 0)]
    for j in range(1, n_cols):
        if j + 1 < n_cols:
            plan.append((0.25 + 0.25 * j, gather.relay_z, j + 1))
        plan.append((0.25 + 0.3 * j, gather.relay_single, j))
        plan.append((0.25 + 0.4 * j, gather.relay_multi, j - 1))
    plan.append((2.0, gather.relay_multi, n_cols - 1))
    for when, act, j in plan:
        if when < 1.0:
            early.setdefault(max(0, int(when * steps) - 1), []).append((act, j))
        else:
            late.setdefault(len(late), (act, j))
    late = [late[i] for i in range(len(late))]

    for part in range(batches):
        fold[...] = jnp.zeros_like(fold)

        def chunk(i, carry, part=part):
            def eight(k, carry):
                first = pl.multiple_of(i * CHUNK + k * 8, 8)
                spread(pl.multiple_of(part * batch + first, 8), first)
                return carry

            lax.fori_loop(0, CHUNK // 8, eight, 0, unroll=True)
            if part == 0:
                for step, acts in early.items():

                    @pl.when(i == step)
                    def _():
                        for act, j in acts:
                            act(j)

            return carry

        lax.fori_loop(0, steps, chunk, 0)
        for j in range(n_cols):
            if part == 0:
                while (gather.relay_multi, j) in late:
                    act, k = late.pop(0)
                    act(k)
                gather.arrived(j)
                gram_slot(j)
            fold_slot(j)
        scatter(part)
    gather.end()


def fold_rows(count, values, length, third, second, owner, both, n_rows, n_cols, third_rows, slab):
    nblk, width = values.shape
    block, span = both.shape
    rank = block * n_rows
    n_hi = n_cols * third_rows // LO
    batch = nblk
    while n_hi * (batch + 8) * LO * 4 > 20 * 1024 * 1024:
        batch //= 2
    vmem = pl.BlockSpec(memory_space=pltpu.VMEM)
    return pl.pallas_call(
        functools.partial(fold_kernel, n_rows, n_cols, third_rows, batch),
        in_specs=[pl.BlockSpec(memory_space=pltpu.SMEM)] + [vmem] * 6,
        out_specs=[vmem] * 3,
        out_shape=[jax.ShapeDtypeStruct((rank, slab), F32)] + [jax.ShapeDtypeStruct((rank, rank), F32)] * 2,
        scratch_shapes=[
            pltpu.VMEM((n_cols, rank, span), BF),
            pltpu.VMEM((n_hi, batch + 8, LO), F32),
            pltpu.VMEM((nblk, width), F32),
            pltpu.VMEM((nblk, width), jnp.int32),
            pltpu.VMEM((batch, rank), F32),
            pltpu.VMEM((nblk, 128), jnp.int32),
            pltpu.SemaphoreType.DMA((2, n_cols)),
            pltpu.SemaphoreType.DMA((n_cols,)),
            pltpu.SemaphoreType.DMA((n_rows // 2, n_cols, 2)),
            pltpu.SemaphoreType.DMA((n_rows // 2, n_cols, 2)),
            pltpu.SemaphoreType.DMA((n_rows // 2, n_cols)),
            pltpu.SemaphoreType.DMA((n_rows // 2, n_cols)),
        ],
        compiler_params=pltpu.CompilerParams(
            vmem_limit_bytes=58 * 1024 * 1024, collective_id=0, has_side_effects=True
        ),
        name="gather_fold",
    )(count, values, length, third, second, owner, both)


def small_inverse(block):
    n = block.shape[0]
    down = lax.broadcasted_iota(jnp.int32, (n, n), 0)
    across = lax.broadcasted_iota(jnp.int32, (n, n), 1)
    for j in range(n):
        column = block[:, j : j + 1]
        pivot = 1.0 / block[j : j + 1, j : j + 1]
        cleared = jnp.where(across == j, jnp.where(down == j, 1.0, 0.0), block)
        row = cleared[j : j + 1, :] * pivot
        block = jnp.where(down == j, row, cleared - column * row)
    return block


def full_inverse(a, size):
    rank = a.shape[0]
    down = lax.broadcasted_iota(jnp.int32, (rank, size), 0)
    eye = jnp.where(
        lax.broadcasted_iota(jnp.int32, (size, size), 0) == lax.broadcasted_iota(jnp.int32, (size, size), 1), 1.0, 0.0
    )
    for k in range(rank // size):
        s, e = k * size, (k + 1) * size
        inverse = small_inverse(a[s:e, s:e])
        column = jnp.where((down >= s) & (down < e), 0.0, a[:, s:e])
        pieces = [a[s:e, :s]] * (s > 0) + [eye] + [a[s:e, e:]] * (e < rank)
        row = dot(inverse, jnp.concatenate(pieces, axis=1), NN, EXACT)
        zero = jnp.zeros((rank, size), F32)
        pieces = [a[:, :s]] * (s > 0) + [zero] + [a[:, e:]] * (e < rank)
        a = jnp.concatenate(pieces, axis=1) - dot(column, row, NN, EXACT)
        pieces = [a[:s]] * (s > 0) + [row] + [a[e:]] * (e < rank)
        a = jnp.concatenate(pieces, axis=0)
    return a


def reach(x):
    return jnp.max(jnp.sum(jnp.abs(x), axis=1, keepdims=True))


def solve_kernel(size, scale, left_ref, right_ref, rows_ref, out_ref, power):
    rank = left_ref.shape[1]
    a = (left_ref[...] / scale[0]) * (right_ref[...] / scale[1])
    down = lax.broadcasted_iota(jnp.int32, (rank, rank), 0)
    across = lax.broadcasted_iota(jnp.int32, (rank, rank), 1)
    diagonal = jnp.where(down == across, a, 0.0)
    down_scale = lax.rsqrt(jnp.sum(diagonal, axis=1, keepdims=True))
    across_scale = lax.rsqrt(jnp.sum(diagonal, axis=0, keepdims=True))
    off = (a * down_scale) * across_scale - jnp.where(down == across, 1.0, 0.0)
    near = reach(off) < 0.5

    @pl.when(near)
    def _():
        square = dot(off, off, NN, EXACT)
        rows = rows_ref[...] * down_scale
        rows = rows - dot(off, rows, NN, EXACT)
        rows = rows + dot(square, rows, NN, EXACT)
        out_ref[...] = rows * down_scale
        power[...] = square

        def more(left):
            return left * left > 1e-9

        def factor(left):
            square = dot(power[...], power[...], NN, EXACT)
            power[...] = square
            rows = out_ref[...] / down_scale
            out_ref[...] = (rows + dot(square, rows, NN, EXACT)) * down_scale
            return reach(square)

        lax.while_loop(more, factor, reach(square))

    @pl.when(jnp.logical_not(near))
    def _():
        out_ref[...] = dot(full_inverse(a, size), rows_ref[...], NN, EXACT)


def solve(left, right, rows, scale):
    return pl.pallas_call(
        functools.partial(solve_kernel, 32, scale),
        out_shape=jax.ShapeDtypeStruct(rows.shape, F32),
        in_specs=[pl.BlockSpec(memory_space=pltpu.VMEM)] * 3,
        out_specs=pl.BlockSpec(memory_space=pltpu.VMEM),
        scratch_shapes=[pltpu.VMEM(left.shape, F32)],
        name="solve",
    )(left, right, rows)


def exchange_kernel(n_rows, n_cols, tiles_ref, out_ref, landed, send, land):
    row, col = lax.axis_index("rows"), lax.axis_index("cols")
    share = n_rows // n_cols
    block = tiles_ref.shape[0] // n_rows
    slab = tiles_ref.shape[1]
    mine = lax.rem(row, share) * n_cols + col
    home = row // share
    stays = home == col
    barrier = pltpu.get_barrier_semaphore()
    for i in range(share):
        for c in range(n_cols):
            source = col * share + i

            @pl.when((source != row) | (c != col))
            def _():
                pl.semaphore_signal(barrier, inc=1, device_id=(source, c), device_id_type=MESH)

    pl.when(stays)(lambda: pl.semaphore_wait(barrier, n_rows - 1))
    pl.when(jnp.logical_not(stays))(lambda: pl.semaphore_wait(barrier, n_rows))

    def copy(flip):
        return pltpu.make_async_remote_copy(
            src_ref=tiles_ref.at[pl.ds(flip * block, block), :],
            dst_ref=landed.at[mine],
            send_sem=send.at[flip],
            recv_sem=land.at[mine],
            device_id=(flipped(row, flip), home),
            device_id_type=MESH,
        )

    order = list(range(n_rows - 1, -1, -1))
    for flip in order:
        if flip:
            copy(flip).start()
        else:
            pl.when(jnp.logical_not(stays))(copy(0).start)

    @pl.when(stays)
    def _():
        landed[mine] = tiles_ref[0:block, :]

    def arrive(i):
        return pltpu.make_async_copy(tiles_ref.at[pl.ds(0, block), :], landed.at[i], land.at[i])

    for i in range(share):
        for c in range(n_cols):
            at = i * n_cols + c
            pl.when(jnp.logical_not(stays & (mine == at)))(arrive(at).wait)
        total = landed[i * n_cols]
        for c in range(1, n_cols):
            total = total + landed[i * n_cols + c]
        out_ref[i * slab : (i + 1) * slab, :] = total.T
    for flip in order:
        if flip:
            copy(flip).wait_send()
        else:
            pl.when(jnp.logical_not(stays))(copy(0).wait_send)


def exchange(tiles, n_rows, n_cols):
    rank, slab = tiles.shape
    block = rank // n_rows
    return pl.pallas_call(
        functools.partial(exchange_kernel, n_rows, n_cols),
        in_specs=[pl.BlockSpec(memory_space=pltpu.VMEM)],
        out_specs=pl.BlockSpec(memory_space=pltpu.VMEM),
        out_shape=jax.ShapeDtypeStruct((n_rows // n_cols * slab, block), F32),
        scratch_shapes=[
            pltpu.VMEM((n_rows, block, slab), F32),
            pltpu.SemaphoreType.DMA((n_rows,)),
            pltpu.SemaphoreType.DMA((n_rows,)),
        ],
        compiler_params=pltpu.CompilerParams(collective_id=1, has_side_effects=True),
        name="exchange",
    )(tiles)


def per_device(
    block_values,
    block_length,
    block_owner,
    block_second,
    block_third,
    live_blocks,
    second_factor,
    third_factor,
):
    n_rows = lax.axis_size("rows")
    n_cols = lax.axis_size("cols")
    nblk = block_values.shape[0]
    range_rows = second_factor.shape[0]
    third_rows = third_factor.shape[0]
    slab = range_rows * n_cols // n_rows
    both = jnp.concatenate([third_factor.T, second_factor.T], axis=1)
    rows, gram_second, gram_third = fold_rows(
        live_blocks,
        block_values,
        block_length.reshape(1, nblk),
        block_third,
        block_second.reshape(1, nblk),
        block_owner.reshape(1, nblk),
        both,
        n_rows,
        n_cols,
        third_rows,
        slab,
    )
    solved = solve(gram_second, gram_third, rows, (range_rows * n_cols, third_rows * n_cols))
    return exchange(solved, n_rows, n_cols)


def solution(mesh):
    return jax.shard_map(
        per_device,
        mesh=mesh,
        in_specs=(
            P(("rows", "cols"), None),
            P(("rows", "cols")),
            P(("rows", "cols")),
            P(("rows", "cols")),
            P(("rows", "cols"), None),
            P(("rows", "cols")),
            P("cols", "rows"),
            P("cols", "rows"),
        ),
        out_specs=P("cols", "rows"),
        check_vma=False,
    )
```

```python
import functools

import jax
import jax.numpy as jnp
from jax import lax
from jax.experimental import pallas as pl
from jax.experimental.pallas import tpu as pltpu
from jax.sharding import PartitionSpec as P

LO = 128
TILE = 256
CHUNK = 32
BF = jnp.bfloat16
F32 = jnp.float32
NT = (((1,), (1,)), ((), ()))
NN = (((1,), (0,)), ((), ()))
EXACT = lax.Precision.HIGHEST
MESH = pl.DeviceIdType.MESH


def dot(a, b, dims, precision=None):
    return lax.dot_general(a, b, dims, precision=precision, preferred_element_type=F32)


def flipped(row, flip):
    target = row
    bit = 1
    while bit <= flip:
        if flip & bit:
            target = target + bit - 2 * bit * lax.rem(row // bit, 2)
        bit *= 2
    return target


class Gather:
    def __init__(self, n_rows, n_cols, third, second, gram, sems):
        self.n_rows, self.n_cols = n_rows, n_cols
        self.third, self.second, self.gram = third, second, gram
        self.send_z, self.land_z, self.send_f, self.land_f, self.hand, self.take = sems
        self.rank = second.shape[0] // n_rows
        self.row, self.col = lax.axis_index("rows"), lax.axis_index("cols")
        self.partner = flipped(self.row, 1)
        self.bits = [b for b in (2**i for i in range(1, 16)) if b < n_rows]
        self.multi = [f for f in range(2, n_rows, 2) if f not in self.bits]
        orders = []
        for c in range(n_cols):
            others = [(abs(a - c), a - c) for a in range(n_cols)]
            orders.append([d for _, d in sorted(others)])
        self.delta = [sum((self.col == c).astype(jnp.int32) * orders[c][j] for c in range(n_cols)) for j in range(n_cols)]
        self.slot = [lax.rem(d + n_cols, n_cols) for d in self.delta] + [n_cols, n_cols + 1]

    def rows(self, block, half=None):
        start = flipped(self.row, block) * self.rank
        size = self.rank
        if half is not None:
            size = self.rank // 2
            start = start + half * size
        return pl.ds(pl.multiple_of(start, size), size)

    def area(self, block, j, half=None):
        if j == self.n_cols:
            return self.second.at[self.rows(block, half), :]
        if j == self.n_cols + 1:
            return self.gram.at[self.rows(block, half), :]
        return self.third.at[self.slot[j], self.rows(block, half), :]

    def z_copy(self, j, up):
        step = 1 if up else -1
        there = lax.rem(self.slot[j] - step + self.n_cols, self.n_cols)
        target = lax.rem(self.col + step + self.n_cols, self.n_cols)
        return pltpu.make_async_remote_copy(
            src_ref=self.area(0, j),
            dst_ref=self.third.at[there, self.rows(0), :],
            send_sem=self.send_z.at[int(up), j],
            recv_sem=self.land_z.at[there],
            device_id=(self.row, target),
            device_id_type=MESH,
        )

    def z_moves(self, j):
        yield True, (self.delta[j] <= 0) & (self.col + 1 < self.n_cols)
        yield False, (self.delta[j] >= 0) & (self.col >= 1)

    def flip_copy(self, bit, block, j, half):
        there = block ^ bit
        part = None if there == bit else half
        return pltpu.make_async_remote_copy(
            src_ref=self.area(block, j, part),
            dst_ref=self.area(block, j, part),
            send_sem=self.send_f.at[there // 2, j, half],
            recv_sem=self.land_f.at[there // 2, self.slot[j], half],
            device_id=(flipped(self.row, bit), self.col),
            device_id_type=MESH,
        )

    def route(self, flip, half):
        bits = [b for b in self.bits if flip & b]
        return bits[0] if half == 0 else bits[-1]

    def core_copy(self, block, j):
        return pltpu.make_async_remote_copy(
            src_ref=self.area(block, j),
            dst_ref=self.area(block, j),
            send_sem=self.hand.at[block // 2, j],
            recv_sem=self.take.at[block // 2, self.slot[j]],
            device_id=(self.partner, self.col),
            device_id_type=MESH,
        )

    def signal(self):
        barrier = pltpu.get_barrier_semaphore()
        near = [(self.partner, self.col)]
        near += [(self.row, lax.rem(self.col + d, self.n_cols)) for d in range(1, self.n_cols)]
        near += [(flipped(self.row, f), self.col) for f in range(2, self.n_rows, 2)]
        for target in near:
            pl.semaphore_signal(barrier, inc=1, device_id=target, device_id_type=MESH)
        return functools.partial(pl.semaphore_wait, barrier, len(near))

    def own_z(self, j):
        for up, there in self.z_moves(j):
            pl.when(there)(self.z_copy(j, up).start)

    def own_flips(self, j):
        for bit in self.bits:
            self.flip_copy(bit, 0, j, 0).start()
        self.core_copy(0, j).start()

    def relay_z(self, j):
        self.z_copy_in(j).wait_recv()
        self.own_z(j)
        self.own_flips(j)

    def z_copy_in(self, j):
        return pltpu.make_async_remote_copy(
            src_ref=self.area(0, j),
            dst_ref=self.area(0, j),
            send_sem=self.send_z.at[0, j],
            recv_sem=self.land_z.at[self.slot[j]],
            device_id=(self.row, lax.rem(self.col + 1, self.n_cols)),
            device_id_type=MESH,
        )

    def relay_single(self, j):
        for block in self.bits:
            self.flip_copy(block, 0, j, 0).wait_recv()
            for flip in self.multi:
                for half in range(2):
                    bit = self.route(flip, half)
                    if flip ^ bit == block:
                        self.flip_copy(bit, block, j, half).start()
            self.core_copy(block, j).start()

    def relay_multi(self, j):
        for block in self.multi:
            for half in range(2):
                bit = self.route(block, half)
                self.flip_copy(bit, block ^ bit, j, half).wait_recv()
                for flip in self.multi:
                    bit = self.route(flip, half)
                    if flip ^ bit == block:
                        self.flip_copy(bit, block, j, half).start()
            self.core_copy(block, j).start()

    def arrived(self, j):
        for block in range(0, self.n_rows, 2):
            self.core_copy(block, j).wait_recv()

    def end(self):
        for j in range(self.n_cols):
            for up, there in self.z_moves(j):
                pl.when(there)(self.z_copy(j, up).wait_send)
        for j in range(self.n_cols + 2):
            for bit in self.bits:
                self.flip_copy(bit, 0, j, 0).wait_send()
            for block in range(0, self.n_rows, 2):
                self.core_copy(block, j).wait_send()
                if block in self.multi:
                    for half in range(2):
                        bit = self.route(block, half)
                        self.flip_copy(bit, block ^ bit, j, half).wait_send()


def fold_kernel(batch, n_rows, n_cols, *refs):
    count_ref, values_in, length_in, third_in, pick_in, owner_in, third_block, second_block = refs[:8]
    out_ref, gram_second_ref, gram_ref, third, second, part_ref, landed = refs[8:15]
    dense, masked, index, fold, values, length, pick_row, owner_row, part_send, part_land, local = refs[15:26]
    gather = Gather(n_rows, n_cols, third, second, gram_second_ref, refs[26:])
    nblk, width = values.shape
    rank, range_rows = second.shape
    third_rows = third.shape[2]
    n_hi = n_cols * third_rows // LO
    part_hi = third_rows // LO
    row, col = gather.row, gather.col
    batches = nblk // batch
    s_piece, g_piece = n_cols, n_cols + 1

    ready = gather.signal()
    sources = [second_block, third_block, values_in, length_in, third_in, pick_in, owner_in]
    targets = [gather.area(0, s_piece), gather.area(0, 0), values, length, index, pick_row, owner_row]
    loads = [pltpu.make_async_copy(a, b, local.at[i]) for i, (a, b) in enumerate(zip(sources, targets))]
    for load in loads:
        load.start()
    ready()
    loads[0].wait()
    gather.own_flips(s_piece)
    loads[1].wait()
    gather.own_z(0)
    gather.own_flips(0)
    for load in loads[2:]:
        load.wait()

    gram_ref[...] = jnp.zeros_like(gram_ref)
    out_ref[...] = jnp.zeros_like(out_ref)
    lane = lax.broadcasted_iota(jnp.int32, (128, width), 1)
    at_slot = lax.broadcasted_iota(jnp.int32, (128, width), 0)
    for i in range(0, nblk, 128):
        blocks = slice(i, i + 128)
        lengths = jnp.broadcast_to(length[:, blocks], (128, 128)).T
        live = (lane < lengths) & (at_slot + i < count_ref[0])
        masked[blocks, :] = jnp.where(live, values[blocks, :].astype(F32), 0.0)
    turned = index[...] - col * third_rows
    index[...] = jnp.where(turned < 0, turned + n_cols * third_rows, turned)

    at = lax.broadcasted_iota(jnp.int32, (max(LO, n_hi), width), 0).astype(F32).astype(BF)
    one = jnp.ones((16, width), BF)
    zero = jnp.zeros((16, width), BF)

    def spread(start, first):
        place = index[pl.ds(start, 8), :]
        value = masked[pl.ds(start, 8), :]
        high = lax.shift_right_logical(place, 7).astype(F32)
        low = (place & (LO - 1)).astype(F32)
        for j in range(8):
            high16 = jnp.broadcast_to(high[j : j + 1, :], (16, width)).astype(BF)
            low16 = jnp.broadcast_to(low[j : j + 1, :], (16, width)).astype(BF)
            value16 = jnp.broadcast_to(value[j : j + 1, :], (16, width)).astype(BF)
            left = [jnp.where(at[k : k + 16] == high16, value16, zero) for k in range(0, n_hi, 16)]
            right = [jnp.where(at[k : k + 16] == low16, one, zero) for k in range(0, LO, 16)]
            tile = dot(jnp.concatenate(left, axis=0), jnp.concatenate(right, axis=0), NT)
            dense[:, pl.ds(first + j, 1), :] = tile.reshape(n_hi, 1, LO)

    def fold_slot(j):
        slot = gather.slot[j]
        per = 4

        def tiles(i, carry):
            total = fold[...]
            for k in range(per):
                at_hi = slot * part_hi + (i * per + k) * (TILE // LO)
                x = jnp.concatenate([dense[at_hi + h, 0:batch, :] for h in range(TILE // LO)], axis=1)
                high = x.astype(BF)
                low = (x - high.astype(F32)).astype(BF)
                start = pl.multiple_of((i * per + k) * TILE, TILE)
                piece = third[slot, :, pl.ds(start, TILE)]
                total = total + (dot(high, piece, NT) + dot(low, piece, NT))
            fold[...] = total
            return carry

        lax.fori_loop(0, third_rows // TILE // per, tiles, 0)

    def gram_slot(j):
        piece = third[gather.slot[j]]
        gram_ref[...] += dot(piece, piece, NT)

    def part_copy(step):
        return pltpu.make_async_remote_copy(
            src_ref=part_ref,
            dst_ref=landed.at[n_cols - step],
            send_sem=part_send.at[step],
            recv_sem=part_land.at[n_cols - step],
            device_id=(row, lax.rem(col + step, n_cols)),
            device_id_type=MESH,
        )

    def part_make(_):
        gather.arrived(s_piece)
        part_ref[...] = dot(second[gather.rows(0), :], second[...], NT)

    def part_start(_):
        for step in range(1, n_cols):
            part_copy(step).start()

    def part_sum(_):
        total = part_ref[...]
        for step in range(1, n_cols):
            part_copy(step).wait_recv()
        for at_col in range(1, n_cols):
            total = total + landed[at_col]
        gram_second_ref[gather.rows(0), :] = total

    def scatter(part):
        columns = slice(part * batch, (part + 1) * batch)
        at_second = lax.broadcasted_iota(jnp.int32, (range_rows, batch), 0) + col * range_rows
        pick = jnp.where(at_second == pick_row[:, columns], 1.0, 0.0).astype(BF)
        contrib = dot(second[...], pick, NN) * fold[...].T
        slab = out_ref.shape[1]
        at_owner = lax.broadcasted_iota(jnp.int32, (slab, batch), 0) + row * slab
        place = jnp.where(at_owner == owner_row[:, columns], 1.0, 0.0).astype(BF)
        high = contrib.astype(BF)
        rest = contrib - high.astype(F32)
        middle = rest.astype(BF)
        low = (rest - middle.astype(F32)).astype(BF)
        out_ref[...] += dot(high, place, NT) + (dot(middle, place, NT) + dot(low, place, NT))

    plan = [
        (3, gather.relay_single, s_piece),
        (6, gather.relay_single, 0),
        (7, gather.relay_multi, s_piece),
        (8, part_make, None),
        (10, part_start, None),
        (14.6, part_sum, None),
        (4.5 * n_cols + 0.5, gather.own_flips, g_piece),
        (4.5 * n_cols + 3, gather.relay_single, g_piece),
    ]
    for j in range(n_cols):
        if j > 0:
            plan.append((4.5 * j, gather.relay_z, j))
            plan.append((4.5 * j + 4.5, gather.relay_single, j))
        plan.append((10.8 + 4.2 * j, gather.relay_multi, j))
    plan.sort(key=lambda entry: entry[0])
    steps = batch // CHUNK
    early = {}
    for when, act, j in plan:
        if when < 16:
            early.setdefault(max(0, int(when / 16 * steps) - 1), []).append((act, j))
    late = [entry for entry in plan if entry[0] >= 16]

    for part in range(batches):
        fold[...] = jnp.zeros_like(fold)

        def chunk(i, carry, part=part):
            def eight(k, carry):
                first = pl.multiple_of(i * CHUNK + k * 8, 8)
                spread(pl.multiple_of(part * batch + first, 8), first)
                return carry

            lax.fori_loop(0, CHUNK // 8, eight, 0, unroll=True)
            if part == 0:
                for step, acts in early.items():

                    @pl.when(i == step)
                    def _():
                        for act, j in acts:
                            act(j)

            return carry

        lax.fori_loop(0, steps, chunk, 0)
        for j in range(n_cols):
            if part == 0:
                due = 16.6 + 1.5 * j
                while late and (late[0][0] <= due or (gather.relay_multi, j) in [entry[1:] for entry in late]):
                    when, act, k = late.pop(0)
                    act(k)
                gather.arrived(j)
                gram_slot(j)
            fold_slot(j)
        scatter(part)
        while late:
            when, act, k = late.pop(0)
            act(k)
    gather.relay_multi(g_piece)
    gather.arrived(g_piece)
    for step in range(1, n_cols):
        part_copy(step).wait_send()
    gather.end()


def fold_rows(count, values, length, third, second, owner, third_block, second_block, n_rows, n_cols, slab):
    nblk, width = values.shape
    block, third_rows = third_block.shape
    range_rows = second_block.shape[1]
    rank = block * n_rows
    n_hi = n_cols * third_rows // LO
    batch = nblk
    while n_hi * (batch + 8) * LO * 4 > 20 * 1024 * 1024:
        batch //= 2
    vmem = pl.BlockSpec(memory_space=pltpu.VMEM)
    dma = pltpu.SemaphoreType.DMA
    return pl.pallas_call(
        functools.partial(fold_kernel, batch, n_rows, n_cols),
        in_specs=[pl.BlockSpec(memory_space=pltpu.SMEM)] + [pl.BlockSpec(memory_space=pltpu.HBM)] * 7,
        out_specs=[vmem] * 3,
        out_shape=[jax.ShapeDtypeStruct((rank, slab), F32)] + [jax.ShapeDtypeStruct((rank, rank), F32)] * 2,
        scratch_shapes=[
            pltpu.VMEM((n_cols, rank, third_rows), BF),
            pltpu.VMEM((rank, range_rows), BF),
            pltpu.VMEM((block, rank), F32),
            pltpu.VMEM((n_cols, block, rank), F32),
            pltpu.VMEM((n_hi, batch + 8, LO), F32),
            pltpu.VMEM((nblk, width), F32),
            pltpu.VMEM((nblk, width), jnp.int32),
            pltpu.VMEM((batch, rank), F32),
            pltpu.VMEM((nblk, width), BF),
            pltpu.VMEM((1, nblk), jnp.int32),
            pltpu.VMEM((1, nblk), jnp.int32),
            pltpu.VMEM((1, nblk), jnp.int32),
            dma((n_cols,)),
            dma((n_cols,)),
            dma((7,)),
            dma((2, n_cols)),
            dma((n_cols,)),
            dma((n_rows // 2, n_cols + 2, 2)),
            dma((n_rows // 2, n_cols + 2, 2)),
            dma((n_rows // 2, n_cols + 2)),
            dma((n_rows // 2, n_cols + 2)),
        ],
        compiler_params=pltpu.CompilerParams(
            vmem_limit_bytes=(40 if batch == nblk else 58) * 1024 * 1024, collective_id=0, has_side_effects=True
        ),
        name="gather_fold",
    )(count, values, length, third, second, owner, third_block, second_block)


def small_inverse(block):
    n = block.shape[0]
    down = lax.broadcasted_iota(jnp.int32, (n, n), 0)
    across = lax.broadcasted_iota(jnp.int32, (n, n), 1)
    for j in range(n):
        column = block[:, j : j + 1]
        pivot = 1.0 / block[j : j + 1, j : j + 1]
        cleared = jnp.where(across == j, jnp.where(down == j, 1.0, 0.0), block)
        row = cleared[j : j + 1, :] * pivot
        block = jnp.where(down == j, row, cleared - column * row)
    return block


def full_inverse(a, size):
    rank = a.shape[0]
    down = lax.broadcasted_iota(jnp.int32, (rank, size), 0)
    eye = jnp.where(
        lax.broadcasted_iota(jnp.int32, (size, size), 0) == lax.broadcasted_iota(jnp.int32, (size, size), 1), 1.0, 0.0
    )
    for k in range(rank // size):
        s, e = k * size, (k + 1) * size
        inverse = small_inverse(a[s:e, s:e])
        column = jnp.where((down >= s) & (down < e), 0.0, a[:, s:e])
        pieces = [a[s:e, :s]] * (s > 0) + [eye] + [a[s:e, e:]] * (e < rank)
        row = dot(inverse, jnp.concatenate(pieces, axis=1), NN, EXACT)
        zero = jnp.zeros((rank, size), F32)
        pieces = [a[:, :s]] * (s > 0) + [zero] + [a[:, e:]] * (e < rank)
        a = jnp.concatenate(pieces, axis=1) - dot(column, row, NN, EXACT)
        pieces = [a[:s]] * (s > 0) + [row] + [a[e:]] * (e < rank)
        a = jnp.concatenate(pieces, axis=0)
    return a


def reach(x):
    return jnp.max(jnp.sum(jnp.abs(x), axis=1, keepdims=True))


def solve_kernel(size, scale, left_ref, right_ref, rows_ref, out_ref, power):
    rank = left_ref.shape[1]
    a = (left_ref[...] / scale[0]) * (right_ref[...] / scale[1])
    down = lax.broadcasted_iota(jnp.int32, (rank, rank), 0)
    across = lax.broadcasted_iota(jnp.int32, (rank, rank), 1)
    diagonal = jnp.where(down == across, a, 0.0)
    down_scale = lax.rsqrt(jnp.sum(diagonal, axis=1, keepdims=True))
    across_scale = lax.rsqrt(jnp.sum(diagonal, axis=0, keepdims=True))
    off = (a * down_scale) * across_scale - jnp.where(down == across, 1.0, 0.0)
    near = reach(off) < 0.5

    @pl.when(near)
    def _():
        square = dot(off, off, NN, EXACT)
        rows = rows_ref[...] * down_scale
        rows = rows - dot(off, rows, NN, EXACT)
        rows = rows + dot(square, rows, NN, EXACT)
        out_ref[...] = rows * down_scale
        power[...] = square

        def more(left):
            return left * left > 1e-9

        def factor(left):
            square = dot(power[...], power[...], NN, EXACT)
            power[...] = square
            rows = out_ref[...] / down_scale
            out_ref[...] = (rows + dot(square, rows, NN, EXACT)) * down_scale
            return reach(square)

        lax.while_loop(more, factor, reach(square))

    @pl.when(jnp.logical_not(near))
    def _():
        out_ref[...] = dot(full_inverse(a, size), rows_ref[...], NN, EXACT)


def solve(left, right, rows, scale):
    return pl.pallas_call(
        functools.partial(solve_kernel, 32, scale),
        out_shape=jax.ShapeDtypeStruct(rows.shape, F32),
        in_specs=[pl.BlockSpec(memory_space=pltpu.VMEM)] * 3,
        out_specs=pl.BlockSpec(memory_space=pltpu.VMEM),
        scratch_shapes=[pltpu.VMEM(left.shape, F32)],
        name="solve",
    )(left, right, rows)


def exchange_kernel(n_rows, n_cols, tiles_ref, out_ref, middle, landed, send_a, land_a, send_b, land_b):
    row, col = lax.axis_index("rows"), lax.axis_index("cols")
    share = n_rows // n_cols
    block = tiles_ref.shape[0] // n_rows
    slab = tiles_ref.shape[1]
    barrier = pltpu.get_barrier_semaphore()
    near = [(flipped(row, f), col) for f in range(1, n_rows)]
    near += [(row, lax.rem(col + d, n_cols)) for d in range(1, n_cols)]
    for target in near:
        pl.semaphore_signal(barrier, inc=1, device_id=target, device_id_type=MESH)
    pl.semaphore_wait(barrier, len(near))

    def tile(flip):
        start = pl.multiple_of(flipped(row, flip) * block, block)
        return tiles_ref.at[pl.ds(start, block), :]

    def across(flip):
        return pltpu.make_async_remote_copy(
            src_ref=tile(flip),
            dst_ref=middle.at[flip],
            send_sem=send_a.at[flip],
            recv_sem=land_a.at[flip],
            device_id=(flipped(row, flip), col),
            device_id_type=MESH,
        )

    def along(flip):
        source = flipped(row, flip)
        home = source // share
        return home, lax.rem(source, share), pltpu.make_async_remote_copy(
            src_ref=middle.at[flip] if flip else tile(0),
            dst_ref=landed.at[lax.rem(source, share) * n_cols + col],
            send_sem=send_b.at[flip],
            recv_sem=land_b.at[lax.rem(source, share) * n_cols + col],
            device_id=(row, home),
            device_id_type=MESH,
        )

    far = list(range(n_rows // 2, n_rows))
    order = list(range(1, n_rows // 2))
    for flip in far[::-1] + order[::-1]:
        across(flip).start()
    for flip in [0] + [f for f in order if f == 1] + far + [f for f in order if f > 1]:
        if flip:
            across(flip).wait_recv()
        home, at, copy = along(flip)
        pl.when(home != col)(copy.start)

        @pl.when(home == col)
        def _():
            landed[at * n_cols + col] = middle[flip] if flip else tile(0)[...]

    def arrive(at, step):
        source = lax.rem(col + step, n_cols)
        return source, pltpu.make_async_remote_copy(
            src_ref=middle.at[0],
            dst_ref=landed.at[at * n_cols + source],
            send_sem=send_b.at[0],
            recv_sem=land_b.at[at * n_cols + source],
            device_id=(row, source),
            device_id_type=MESH,
        )

    for at in range(share):
        for step in range(1, n_cols):
            arrive(at, step)[1].wait_recv()
        total = landed[at * n_cols]
        for c in range(1, n_cols):
            total = total + landed[at * n_cols + c]
        out_ref[:, at * slab : (at + 1) * slab] = total
    for flip in range(n_rows):
        if flip:
            across(flip).wait_send()
        home, at, copy = along(flip)
        pl.when(home != col)(copy.wait_send)


def exchange(tiles, n_rows, n_cols):
    rank, slab = tiles.shape
    block = rank // n_rows
    dma = pltpu.SemaphoreType.DMA
    return pl.pallas_call(
        functools.partial(exchange_kernel, n_rows, n_cols),
        in_specs=[pl.BlockSpec(memory_space=pltpu.VMEM)],
        out_specs=pl.BlockSpec(memory_space=pltpu.VMEM),
        out_shape=jax.ShapeDtypeStruct((block, n_rows // n_cols * slab), F32),
        scratch_shapes=[pltpu.VMEM((n_rows, block, slab), F32)] * 2 + [dma((n_rows,))] * 4,
        compiler_params=pltpu.CompilerParams(collective_id=1, has_side_effects=True),
        name="exchange",
    )(tiles)


def per_device(
    block_values,
    block_length,
    block_owner,
    block_second,
    block_third,
    live_blocks,
    second_factor,
    third_factor,
):
    n_rows = lax.axis_size("rows")
    n_cols = lax.axis_size("cols")
    nblk = block_values.shape[0]
    range_rows = second_factor.shape[0]
    third_rows = third_factor.shape[0]
    slab = range_rows * n_cols // n_rows
    rows, gram_second, gram_third = fold_rows(
        live_blocks,
        block_values,
        block_length.reshape(1, nblk),
        block_third,
        block_second.reshape(1, nblk),
        block_owner.reshape(1, nblk),
        third_factor.T,
        second_factor.T,
        n_rows,
        n_cols,
        slab,
    )
    solved = solve(gram_second, gram_third, rows, (range_rows * n_cols, third_rows * n_cols))
    return exchange(solved, n_rows, n_cols).T


def solution(mesh):
    return jax.shard_map(
        per_device,
        mesh=mesh,
        in_specs=(
            P(("rows", "cols"), None),
            P(("rows", "cols")),
            P(("rows", "cols")),
            P(("rows", "cols")),
            P(("rows", "cols"), None),
            P(("rows", "cols")),
            P("cols", "rows"),
            P("cols", "rows"),
        ),
        out_specs=P("cols", "rows"),
        check_vma=False,
    )
```

```python
import functools

import jax
import jax.numpy as jnp
from jax import lax
from jax.experimental import pallas as pl
from jax.experimental.pallas import tpu as pltpu
from jax.sharding import PartitionSpec as P

LO = 128
CHUNK = 32
BF = jnp.bfloat16
F32 = jnp.float32
NT = (((1,), (1,)), ((), ()))
NN = (((1,), (0,)), ((), ()))
EXACT = lax.Precision.HIGHEST
MESH = pl.DeviceIdType.MESH


def dot(a, b, dims, precision=None):
    return lax.dot_general(a, b, dims, precision=precision, preferred_element_type=F32)


def flipped(row, flip):
    target = row
    bit = 1
    while bit <= flip:
        if flip & bit:
            target = target + bit - 2 * bit * lax.rem(row // bit, 2)
        bit *= 2
    return target


class Gather:
    def __init__(self, n_rows, n_cols, third, second, gram, sems):
        self.n_rows, self.n_cols = n_rows, n_cols
        self.third, self.second, self.gram = third, second, gram
        self.send_z, self.land_z, self.send_f, self.land_f, self.hand, self.take = sems
        self.rank = second.shape[0] // n_rows
        self.row, self.col = lax.axis_index("rows"), lax.axis_index("cols")
        self.partner = flipped(self.row, 1)
        self.bits = [b for b in (2**i for i in range(1, 16)) if b < n_rows]
        self.multi = [f for f in range(2, n_rows, 2) if f not in self.bits]
        self.near = []
        for c in range(n_cols):
            self.near.append(sorted(range(n_cols), key=lambda a: (abs(a - c), a)))

    def by_col(self, table):
        return sum((self.col == c).astype(jnp.int32) * table[c] for c in range(self.n_cols))

    def position(self, up, k, there=0):
        table = []
        for c in range(self.n_cols):
            source = c - k if up else c + k
            holder = c + there
            known = 0 <= source < self.n_cols and 0 <= holder < self.n_cols
            table.append(self.near[holder].index(source) if known else 0)
        return self.by_col(table)

    def source_of(self, j):
        return self.by_col([self.near[c][j] for c in range(self.n_cols)])

    def rows(self, block, half=None):
        start = flipped(self.row, block) * self.rank
        size = self.rank
        if half is not None:
            size = self.rank // 2
            start = start + half * size
        return pl.ds(pl.multiple_of(start, size), size)

    def area(self, block, j, half=None):
        if isinstance(j, int) and j == self.n_cols:
            return self.second.at[self.rows(block, half), :]
        if isinstance(j, int) and j == self.n_cols + 1:
            return self.gram.at[self.rows(block, half), :]
        return self.third.at[j, self.rows(block, half), :]

    def z_copy(self, up, k, half):
        step = 1 if up else -1
        return pltpu.make_async_remote_copy(
            src_ref=self.area(0, self.position(up, k), half),
            dst_ref=self.area(0, self.position(up, k, step), half),
            send_sem=self.send_z.at[int(up), k, half],
            recv_sem=self.land_z.at[int(up), k, half],
            device_id=(self.row, lax.rem(self.col + step + self.n_cols, self.n_cols)),
            device_id_type=MESH,
        )

    def goes_on(self, up, k):
        return (self.col >= k) & (self.col + 1 < self.n_cols) if up else (self.col + k < self.n_cols) & (self.col >= 1)

    def relay_z(self, k, half):
        for up in (True, False):
            here = self.col >= k if up else self.col + k < self.n_cols

            @pl.when(here)
            def _():
                self.z_copy(up, k - 1, half).wait_recv()

            pl.when(self.goes_on(up, k))(self.z_copy(up, k, half).start)

            @pl.when(here)
            def _():
                self.own_flips(self.position(up, k), half)

    def flip_copy(self, bit, block, j, half):
        there = block ^ bit
        return pltpu.make_async_remote_copy(
            src_ref=self.area(block, j, half),
            dst_ref=self.area(block, j, half),
            send_sem=self.send_f.at[there // 2, j, half],
            recv_sem=self.land_f.at[there // 2, j, half],
            device_id=(flipped(self.row, bit), self.col),
            device_id_type=MESH,
        )

    def route(self, flip, half):
        bits = [b for b in self.bits if flip & b]
        return bits[0] if half == 0 else bits[-1]

    def core_copy(self, block, j, half):
        return pltpu.make_async_remote_copy(
            src_ref=self.area(block, j, half),
            dst_ref=self.area(block, j, half),
            send_sem=self.hand.at[block // 2, j, half],
            recv_sem=self.take.at[block // 2, j, half],
            device_id=(self.partner, self.col),
            device_id_type=MESH,
        )

    def signal(self):
        barrier = pltpu.get_barrier_semaphore()
        near = [(self.partner, self.col)]
        near += [(self.row, lax.rem(self.col + d, self.n_cols)) for d in range(1, self.n_cols)]
        near += [(flipped(self.row, f), self.col) for f in range(2, self.n_rows, 2)]
        for target in near:
            pl.semaphore_signal(barrier, inc=1, device_id=target, device_id_type=MESH)
        return functools.partial(pl.semaphore_wait, barrier, len(near))

    def own_z(self, half):
        for up in (True, False):
            pl.when(self.goes_on(up, 0))(self.z_copy(up, 0, half).start)

    def own_flips(self, j, half):
        for bit in self.bits:
            self.flip_copy(bit, 0, j, half).start()
        self.core_copy(0, j, half).start()

    def pass_on(self, block, j, half):
        for flip in self.multi:
            bit = self.route(flip, half)
            if flip ^ bit == block:
                self.flip_copy(bit, block, j, half).start()
        self.core_copy(block, j, half).start()

    def relay_single(self, j, half):
        for block in self.bits:
            self.flip_copy(block, 0, j, half).wait_recv()
            self.pass_on(block, j, half)

    def relay_multi(self, j, half):
        for block in self.multi:
            bit = self.route(block, half)
            self.flip_copy(bit, block ^ bit, j, half).wait_recv()
            self.pass_on(block, j, half)

    def arrived(self, j):
        for block in range(0, self.n_rows, 2):
            for half in range(2):
                self.core_copy(block, j, half).wait_recv()

    def end(self):
        for half in range(2):
            for k in range(self.n_cols - 1):
                for up in (True, False):
                    pl.when(self.goes_on(up, k))(self.z_copy(up, k, half).wait_send)
            for j in range(self.n_cols + 2):
                for bit in self.bits:
                    self.flip_copy(bit, 0, j, half).wait_send()
                for block in range(0, self.n_rows, 2):
                    self.core_copy(block, j, half).wait_send()
                    if block in self.multi:
                        bit = self.route(block, half)
                        self.flip_copy(bit, block ^ bit, j, half).wait_send()


def fold_kernel(batch, n_rows, n_cols, *refs):
    count_ref, values_in, length_in, third_in, pick_in, owner_in, third_block, second_block = refs[:8]
    out_ref, gram_second_ref, gram_ref, third, second, part_ref, landed = refs[8:15]
    dense, masked, index, fold, values, length, pick_row, owner_row, part_send, part_land, local = refs[15:26]
    gather = Gather(n_rows, n_cols, third, second, gram_second_ref, refs[26:])
    nblk, width = values.shape
    rank, range_rows = second.shape
    third_rows = third.shape[2]
    n_hi = n_cols * third_rows // LO
    part_hi = third_rows // LO
    row, col = gather.row, gather.col
    batches = nblk // batch
    s_piece, g_piece = n_cols, n_cols + 1

    ready = gather.signal()
    sources = [second_block, third_block, values_in, length_in, third_in, pick_in, owner_in]
    targets = [gather.area(0, s_piece), gather.area(0, 0), values, length, index, pick_row, owner_row]
    loads = [pltpu.make_async_copy(a, b, local.at[i]) for i, (a, b) in enumerate(zip(sources, targets))]
    for load in loads:
        load.start()
    ready()
    loads[0].wait()
    for half in range(2):
        gather.own_flips(s_piece, half)
    loads[1].wait()
    for half in range(2):
        gather.own_z(half)
        gather.own_flips(0, half)
    for load in loads[2:]:
        load.wait()

    gram_ref[...] = jnp.zeros_like(gram_ref)
    out_ref[...] = jnp.zeros_like(out_ref)
    lane = lax.broadcasted_iota(jnp.int32, (128, width), 1)
    at_slot = lax.broadcasted_iota(jnp.int32, (128, width), 0)
    for i in range(0, nblk, 128):
        blocks = slice(i, i + 128)
        lengths = jnp.broadcast_to(length[:, blocks], (128, 128)).T
        live = (lane < lengths) & (at_slot + i < count_ref[0])
        masked[blocks, :] = jnp.where(live, values[blocks, :].astype(F32), 0.0)
    given = index[...]
    turned = given
    for j in range(n_cols):
        start = gather.source_of(j) * third_rows
        inside = (given >= start) & (given < start + third_rows)
        turned = jnp.where(inside, given - start + j * third_rows, turned)
    index[...] = turned

    at = lax.broadcasted_iota(jnp.int32, (max(LO, n_hi), width), 0).astype(F32).astype(BF)
    one = jnp.ones((16, width), BF)
    zero = jnp.zeros((16, width), BF)

    def spread(start, first):
        place = index[pl.ds(start, 8), :]
        value = masked[pl.ds(start, 8), :]
        high = lax.shift_right_logical(place, 7).astype(F32)
        low = (place & (LO - 1)).astype(F32)
        for j in range(8):
            high16 = jnp.broadcast_to(high[j : j + 1, :], (16, width)).astype(BF)
            low16 = jnp.broadcast_to(low[j : j + 1, :], (16, width)).astype(BF)
            value16 = jnp.broadcast_to(value[j : j + 1, :], (16, width)).astype(BF)
            left = [jnp.where(at[k : k + 16] == high16, value16, zero) for k in range(0, n_hi, 16)]
            right = [jnp.where(at[k : k + 16] == low16, one, zero) for k in range(0, LO, 16)]
            tile = dot(jnp.concatenate(left, axis=0), jnp.concatenate(right, axis=0), NT)
            dense[:, pl.ds(first + j, 1), :] = tile.reshape(n_hi, 1, LO)

    def fold_slot(j):
        depth = third_rows // 2
        total = fold[...]
        for k in range(2):
            at_hi = j * part_hi + k * (depth // LO)
            x = jnp.concatenate([dense[at_hi + h, 0:batch, :] for h in range(depth // LO)], axis=1)
            high = x.astype(BF)
            low = (x - high.astype(F32)).astype(BF)
            piece = third[j, :, k * depth : (k + 1) * depth]
            total = total + (dot(high, piece, NT) + dot(low, piece, NT))
        fold[...] = total

    def gram_slot(j):
        piece = third[j]
        gram_ref[...] += dot(piece, piece, NT)

    def part_copy(step):
        return pltpu.make_async_remote_copy(
            src_ref=part_ref,
            dst_ref=landed.at[n_cols - step],
            send_sem=part_send.at[step],
            recv_sem=part_land.at[n_cols - step],
            device_id=(row, lax.rem(col + step, n_cols)),
            device_id_type=MESH,
        )

    def part_make():
        gather.arrived(s_piece)
        part_ref[...] = dot(second[gather.rows(0), :], second[...], NT)

    def part_start():
        for step in range(1, n_cols):
            part_copy(step).start()

    def part_sum():
        total = part_ref[...]
        for step in range(1, n_cols):
            part_copy(step).wait_recv()
        for at_col in range(1, n_cols):
            total = total + landed[at_col]
        gram_second_ref[gather.rows(0), :] = total

    def scatter(part):
        columns = slice(part * batch, (part + 1) * batch)
        at_second = lax.broadcasted_iota(jnp.int32, (range_rows, batch), 0) + col * range_rows
        pick = jnp.where(at_second == pick_row[:, columns], 1.0, 0.0).astype(BF)
        contrib = dot(second[...], pick, NN) * fold[...].T
        slab = out_ref.shape[1]
        at_owner = lax.broadcasted_iota(jnp.int32, (slab, batch), 0) + row * slab
        place = jnp.where(at_owner == owner_row[:, columns], 1.0, 0.0).astype(BF)
        high = contrib.astype(BF)
        rest = contrib - high.astype(F32)
        middle = rest.astype(BF)
        low = (rest - middle.astype(F32)).astype(BF)
        out_ref[...] += dot(high, place, NT) + (dot(middle, place, NT) + dot(low, place, NT))

    plan = [(11.3, part_make, ()), (12.3, part_start, ()), (16.0, part_sum, ())]
    due = []
    last = 4.1 * n_cols + 2
    for half in range(2):
        plan.append((4.8 + 0.1 * half, gather.relay_single, (s_piece, half)))
        plan.append((9.6 + 0.1 * half, gather.relay_multi, (s_piece, half)))
        plan.append((last + 0.1 * half, gather.own_flips, (g_piece, half)))
        plan.append((last + 5.5 + 0.3 * half, gather.relay_single, (g_piece, half)))
        plan.append((last + 8.3 + 0.3 * half, gather.relay_multi, (g_piece, half)))
        for j in range(n_cols):
            single = 6.2 + 1.3 * half
            if j > 0:
                plan.append((4.8 + 3.55 * (j - 1) + 1.4 * half, gather.relay_z, (j, half)))
                single = 9.6 + 4.1 * (j - 1) + 2.8 * half
            multi = max(13.7 + 4.6 * j - 0.62 * j * j, 12.1 + 4.1 * (j - 1)) + 1.2 * half
            multi = max(multi, single + 2.5)
            plan.append((single, gather.relay_single, (j, half)))
            plan.append((multi, gather.relay_multi, (j, half)))
            if half:
                due.append(max(multi + 1.6, 19.5 + 1.7 * j))
    plan.sort(key=lambda entry: entry[0])
    steps = batch // CHUNK
    early = {}
    late = []
    for when, act, args in plan:
        step = max(0, int((when - 2.2) / 16.0 * steps))
        if step < steps:
            early.setdefault(step, []).append((act, args))
        else:
            late.append((when, act, args))

    def dispatch(i, low, high):
        if high - low > 1:
            middle = (low + high) // 2
            pl.when(i < middle)(functools.partial(dispatch, i, low, middle))
            pl.when(i >= middle)(functools.partial(dispatch, i, middle, high))
        else:
            for act, args in early.get(low, []):
                act(*args)

    def catch_up(until):
        while late and late[0][0] <= until:
            when, act, args = late.pop(0)
            act(*args)

    for part in range(batches):
        fold[...] = jnp.zeros_like(fold)

        def chunk(i, carry, part=part):
            def eight(k, carry):
                first = pl.multiple_of(i * CHUNK + k * 8, 8)
                spread(pl.multiple_of(part * batch + first, 8), first)
                return carry

            lax.fori_loop(0, CHUNK // 8, eight, 0, unroll=True)
            if part == 0:
                dispatch(i, 0, steps)

            return carry

        lax.fori_loop(0, steps, chunk, 0)
        for j in range(n_cols):
            if part == 0:
                catch_up(due[j])
                gather.arrived(j)
                gram_slot(j)
            fold_slot(j)
        if part == 0:
            catch_up(due[-1] + 0.5)
        scatter(part)
        catch_up(1000)
    gather.arrived(g_piece)
    for step in range(1, n_cols):
        part_copy(step).wait_send()
    gather.end()


def fold_rows(count, values, length, third, second, owner, third_block, second_block, n_rows, n_cols, slab):
    nblk, width = values.shape
    block, third_rows = third_block.shape
    range_rows = second_block.shape[1]
    rank = block * n_rows
    n_hi = n_cols * third_rows // LO
    batch = nblk
    while n_hi * (batch + 8) * LO * 4 > 20 * 1024 * 1024:
        batch //= 2
    vmem = pl.BlockSpec(memory_space=pltpu.VMEM)
    dma = pltpu.SemaphoreType.DMA
    return pl.pallas_call(
        functools.partial(fold_kernel, batch, n_rows, n_cols),
        in_specs=[pl.BlockSpec(memory_space=pltpu.SMEM)] + [pl.BlockSpec(memory_space=pltpu.HBM)] * 7,
        out_specs=[vmem] * 3,
        out_shape=[jax.ShapeDtypeStruct((rank, slab), F32)] + [jax.ShapeDtypeStruct((rank, rank), F32)] * 2,
        scratch_shapes=[
            pltpu.VMEM((n_cols, rank, third_rows), BF),
            pltpu.VMEM((rank, range_rows), BF),
            pltpu.VMEM((block, rank), F32),
            pltpu.VMEM((n_cols, block, rank), F32),
            pltpu.VMEM((n_hi, batch + 8, LO), F32),
            pltpu.VMEM((nblk, width), F32),
            pltpu.VMEM((nblk, width), jnp.int32),
            pltpu.VMEM((batch, rank), F32),
            pltpu.VMEM((nblk, width), BF),
            pltpu.VMEM((1, nblk), jnp.int32),
            pltpu.VMEM((1, nblk), jnp.int32),
            pltpu.VMEM((1, nblk), jnp.int32),
            dma((n_cols,)),
            dma((n_cols,)),
            dma((7,)),
            dma((2, n_cols, 2)),
            dma((2, n_cols, 2)),
        ]
        + [dma((n_rows // 2, n_cols + 2, 2))] * 4,
        compiler_params=pltpu.CompilerParams(
            vmem_limit_bytes=58 * 1024 * 1024, collective_id=0, has_side_effects=True
        ),
        name="gather_fold",
    )(count, values, length, third, second, owner, third_block, second_block)


def small_inverse(block):
    n = block.shape[0]
    down = lax.broadcasted_iota(jnp.int32, (n, n), 0)
    across = lax.broadcasted_iota(jnp.int32, (n, n), 1)
    for j in range(n):
        column = block[:, j : j + 1]
        pivot = 1.0 / block[j : j + 1, j : j + 1]
        cleared = jnp.where(across == j, jnp.where(down == j, 1.0, 0.0), block)
        row = cleared[j : j + 1, :] * pivot
        block = jnp.where(down == j, row, cleared - column * row)
    return block


def full_inverse(a, size):
    rank = a.shape[0]
    down = lax.broadcasted_iota(jnp.int32, (rank, size), 0)
    eye = jnp.where(
        lax.broadcasted_iota(jnp.int32, (size, size), 0) == lax.broadcasted_iota(jnp.int32, (size, size), 1), 1.0, 0.0
    )
    for k in range(rank // size):
        s, e = k * size, (k + 1) * size
        inverse = small_inverse(a[s:e, s:e])
        column = jnp.where((down >= s) & (down < e), 0.0, a[:, s:e])
        pieces = [a[s:e, :s]] * (s > 0) + [eye] + [a[s:e, e:]] * (e < rank)
        row = dot(inverse, jnp.concatenate(pieces, axis=1), NN, EXACT)
        zero = jnp.zeros((rank, size), F32)
        pieces = [a[:, :s]] * (s > 0) + [zero] + [a[:, e:]] * (e < rank)
        a = jnp.concatenate(pieces, axis=1) - dot(column, row, NN, EXACT)
        pieces = [a[:s]] * (s > 0) + [row] + [a[e:]] * (e < rank)
        a = jnp.concatenate(pieces, axis=0)
    return a


def reach(x):
    return jnp.max(jnp.sum(jnp.abs(x), axis=1, keepdims=True))


def solve_kernel(size, scale, left_ref, right_ref, rows_ref, out_ref, power):
    rank = left_ref.shape[1]
    a = (left_ref[...] / scale[0]) * (right_ref[...] / scale[1])
    down = lax.broadcasted_iota(jnp.int32, (rank, rank), 0)
    across = lax.broadcasted_iota(jnp.int32, (rank, rank), 1)
    diagonal = jnp.where(down == across, a, 0.0)
    down_scale = lax.rsqrt(jnp.sum(diagonal, axis=1, keepdims=True))
    across_scale = lax.rsqrt(jnp.sum(diagonal, axis=0, keepdims=True))
    off = (a * down_scale) * across_scale - jnp.where(down == across, 1.0, 0.0)
    near = reach(off) < 0.5

    @pl.when(near)
    def _():
        square = dot(off, off, NN, EXACT)
        rows = rows_ref[...] * down_scale
        rows = rows - dot(off, rows, NN, EXACT)
        rows = rows + dot(square, rows, NN, EXACT)
        out_ref[...] = rows * down_scale
        power[...] = square

        def more(left):
            return left * left > 1e-9

        def factor(left):
            square = dot(power[...], power[...], NN, EXACT)
            power[...] = square
            rows = out_ref[...] / down_scale
            out_ref[...] = (rows + dot(square, rows, NN, EXACT)) * down_scale
            return reach(square)

        lax.while_loop(more, factor, reach(square))

    @pl.when(jnp.logical_not(near))
    def _():
        out_ref[...] = dot(full_inverse(a, size), rows_ref[...], NN, EXACT)


def solve(left, right, rows, scale):
    return pl.pallas_call(
        functools.partial(solve_kernel, 32, scale),
        out_shape=jax.ShapeDtypeStruct(rows.shape, F32),
        in_specs=[pl.BlockSpec(memory_space=pltpu.VMEM)] * 3,
        out_specs=pl.BlockSpec(memory_space=pltpu.VMEM),
        scratch_shapes=[pltpu.VMEM(left.shape, F32)],
        name="solve",
    )(left, right, rows)


def exchange_kernel(n_rows, n_cols, tiles_ref, out_ref, middle, landed, send_a, land_a, send_b, land_b):
    row, col = lax.axis_index("rows"), lax.axis_index("cols")
    share = n_rows // n_cols
    block = tiles_ref.shape[0] // n_rows
    slab = tiles_ref.shape[1]
    barrier = pltpu.get_barrier_semaphore()
    near = [(flipped(row, f), col) for f in range(1, n_rows)]
    near += [(row, lax.rem(col + d, n_cols)) for d in range(1, n_cols)]
    for target in near:
        pl.semaphore_signal(barrier, inc=1, device_id=target, device_id_type=MESH)
    pl.semaphore_wait(barrier, len(near))

    def tile(flip):
        start = pl.multiple_of(flipped(row, flip) * block, block)
        return tiles_ref.at[pl.ds(start, block), :]

    def across(flip):
        return pltpu.make_async_remote_copy(
            src_ref=tile(flip),
            dst_ref=middle.at[flip],
            send_sem=send_a.at[flip],
            recv_sem=land_a.at[flip],
            device_id=(flipped(row, flip), col),
            device_id_type=MESH,
        )

    def along(flip):
        source = flipped(row, flip)
        home = source // share
        return home, lax.rem(source, share), pltpu.make_async_remote_copy(
            src_ref=middle.at[flip] if flip else tile(0),
            dst_ref=landed.at[lax.rem(source, share) * n_cols + col],
            send_sem=send_b.at[flip],
            recv_sem=land_b.at[lax.rem(source, share) * n_cols + col],
            device_id=(row, home),
            device_id_type=MESH,
        )

    far = list(range(n_rows // 2, n_rows))
    order = list(range(1, n_rows // 2))
    for flip in far[::-1] + order[::-1]:
        across(flip).start()
    for flip in [0] + [f for f in order if f == 1] + far + [f for f in order if f > 1]:
        if flip:
            across(flip).wait_recv()
        home, at, copy = along(flip)
        pl.when(home != col)(copy.start)

        @pl.when(home == col)
        def _():
            landed[at * n_cols + col] = middle[flip] if flip else tile(0)[...]

    def arrive(at, step):
        source = lax.rem(col + step, n_cols)
        return source, pltpu.make_async_remote_copy(
            src_ref=middle.at[0],
            dst_ref=landed.at[at * n_cols + source],
            send_sem=send_b.at[0],
            recv_sem=land_b.at[at * n_cols + source],
            device_id=(row, source),
            device_id_type=MESH,
        )

    for at in range(share):
        for step in range(1, n_cols):
            arrive(at, step)[1].wait_recv()
        total = landed[at * n_cols]
        for c in range(1, n_cols):
            total = total + landed[at * n_cols + c]
        out_ref[:, at * slab : (at + 1) * slab] = total
    for flip in range(n_rows):
        if flip:
            across(flip).wait_send()
        home, at, copy = along(flip)
        pl.when(home != col)(copy.wait_send)


def exchange(tiles, n_rows, n_cols):
    rank, slab = tiles.shape
    block = rank // n_rows
    dma = pltpu.SemaphoreType.DMA
    return pl.pallas_call(
        functools.partial(exchange_kernel, n_rows, n_cols),
        in_specs=[pl.BlockSpec(memory_space=pltpu.VMEM)],
        out_specs=pl.BlockSpec(memory_space=pltpu.VMEM),
        out_shape=jax.ShapeDtypeStruct((block, n_rows // n_cols * slab), F32),
        scratch_shapes=[pltpu.VMEM((n_rows, block, slab), F32)] * 2 + [dma((n_rows,))] * 4,
        compiler_params=pltpu.CompilerParams(collective_id=1, has_side_effects=True),
        name="exchange",
    )(tiles)


def per_device(
    block_values,
    block_length,
    block_owner,
    block_second,
    block_third,
    live_blocks,
    second_factor,
    third_factor,
):
    n_rows = lax.axis_size("rows")
    n_cols = lax.axis_size("cols")
    nblk = block_values.shape[0]
    range_rows = second_factor.shape[0]
    third_rows = third_factor.shape[0]
    slab = range_rows * n_cols // n_rows
    rows, gram_second, gram_third = fold_rows(
        live_blocks,
        block_values,
        block_length.reshape(1, nblk),
        block_third,
        block_second.reshape(1, nblk),
        block_owner.reshape(1, nblk),
        third_factor.T,
        second_factor.T,
        n_rows,
        n_cols,
        slab,
    )
    solved = solve(gram_second, gram_third, rows, (range_rows * n_cols, third_rows * n_cols))
    return exchange(solved, n_rows, n_cols).T


def solution(mesh):
    return jax.shard_map(
        per_device,
        mesh=mesh,
        in_specs=(
            P(("rows", "cols"), None),
            P(("rows", "cols")),
            P(("rows", "cols")),
            P(("rows", "cols")),
            P(("rows", "cols"), None),
            P(("rows", "cols")),
            P("cols", "rows"),
            P("cols", "rows"),
        ),
        out_specs=P("cols", "rows"),
        check_vma=False,
    )
```

```python
import functools

import jax
import jax.numpy as jnp
from jax import lax
from jax.experimental import pallas as pl
from jax.experimental.pallas import tpu as pltpu
from jax.sharding import PartitionSpec as P

LO = 128
CHUNK = 32
BF = jnp.bfloat16
F32 = jnp.float32
NT = (((1,), (1,)), ((), ()))
NN = (((1,), (0,)), ((), ()))
EXACT = lax.Precision.HIGHEST
MESH = pl.DeviceIdType.MESH


def dot(a, b, dims, precision=None):
    return lax.dot_general(a, b, dims, precision=precision, preferred_element_type=F32)


def flipped(row, flip):
    target = row
    bit = 1
    while bit <= flip:
        if flip & bit:
            target = target + bit - 2 * bit * lax.rem(row // bit, 2)
        bit *= 2
    return target


class Gather:
    def __init__(self, n_rows, n_cols, third, second, gram, sems):
        self.n_rows, self.n_cols = n_rows, n_cols
        self.third, self.second, self.gram = third, second, gram
        self.send_z, self.land_z, self.send_f, self.land_f, self.hand, self.take = sems
        self.rank = second.shape[0] // n_rows
        self.row, self.col = lax.axis_index("rows"), lax.axis_index("cols")
        self.partner = flipped(self.row, 1)
        self.bits = [b for b in (2**i for i in range(1, 16)) if b < n_rows]
        self.multi = [f for f in range(2, n_rows, 2) if f not in self.bits]
        self.near = []
        for c in range(n_cols):
            self.near.append(sorted(range(n_cols), key=lambda a: (abs(a - c), a)))

    def by_col(self, table):
        return sum((self.col == c).astype(jnp.int32) * table[c] for c in range(self.n_cols))

    def position(self, up, k, there=0):
        table = []
        for c in range(self.n_cols):
            source = c - k if up else c + k
            holder = c + there
            known = 0 <= source < self.n_cols and 0 <= holder < self.n_cols
            table.append(self.near[holder].index(source) if known else 0)
        return self.by_col(table)

    def source_of(self, j):
        return self.by_col([self.near[c][j] for c in range(self.n_cols)])

    def rows(self, block, half=None):
        start = flipped(self.row, block) * self.rank
        size = self.rank
        if half is not None:
            size = self.rank // 2
            start = start + half * size
        return pl.ds(pl.multiple_of(start, size), size)

    def area(self, block, j, half=None):
        if isinstance(j, int) and j == self.n_cols:
            return self.second.at[self.rows(block, half), :]
        if isinstance(j, int) and j == self.n_cols + 1:
            return self.gram.at[self.rows(block, half), :]
        return self.third.at[j, self.rows(block, half), :]

    def z_copy(self, up, k, half):
        step = 1 if up else -1
        return pltpu.make_async_remote_copy(
            src_ref=self.area(0, self.position(up, k), half),
            dst_ref=self.area(0, self.position(up, k, step), half),
            send_sem=self.send_z.at[int(up), k, half],
            recv_sem=self.land_z.at[int(up), k, half],
            device_id=(self.row, lax.rem(self.col + step + self.n_cols, self.n_cols)),
            device_id_type=MESH,
        )

    def goes_on(self, up, k):
        return (self.col >= k) & (self.col + 1 < self.n_cols) if up else (self.col + k < self.n_cols) & (self.col >= 1)

    def relay_z(self, k, half):
        for up in (True, False):
            here = self.col >= k if up else self.col + k < self.n_cols

            @pl.when(here)
            def _():
                self.z_copy(up, k - 1, half).wait_recv()

            pl.when(self.goes_on(up, k))(self.z_copy(up, k, half).start)

            @pl.when(here)
            def _():
                self.own_flips(self.position(up, k), half)

    def flip_copy(self, bit, block, j, half):
        there = block ^ bit
        return pltpu.make_async_remote_copy(
            src_ref=self.area(block, j, half),
            dst_ref=self.area(block, j, half),
            send_sem=self.send_f.at[there // 2, j, half],
            recv_sem=self.land_f.at[there // 2, j, half],
            device_id=(flipped(self.row, bit), self.col),
            device_id_type=MESH,
        )

    def route(self, flip, half):
        bits = [b for b in self.bits if flip & b]
        return bits[0] if half == 0 else bits[-1]

    def core_copy(self, block, j, half):
        return pltpu.make_async_remote_copy(
            src_ref=self.area(block, j, half),
            dst_ref=self.area(block, j, half),
            send_sem=self.hand.at[block // 2, j, half],
            recv_sem=self.take.at[block // 2, j, half],
            device_id=(self.partner, self.col),
            device_id_type=MESH,
        )

    def signal(self):
        barrier = pltpu.get_barrier_semaphore()
        near = [(self.partner, self.col)]
        near += [(self.row, lax.rem(self.col + d, self.n_cols)) for d in range(1, self.n_cols)]
        near += [(flipped(self.row, f), self.col) for f in range(2, self.n_rows, 2)]
        for target in near:
            pl.semaphore_signal(barrier, inc=1, device_id=target, device_id_type=MESH)
        return functools.partial(pl.semaphore_wait, barrier, len(near))

    def own_z(self, half):
        for up in (True, False):
            pl.when(self.goes_on(up, 0))(self.z_copy(up, 0, half).start)

    def own_flips(self, j, half):
        for bit in self.bits:
            self.flip_copy(bit, 0, j, half).start()
        self.core_copy(0, j, half).start()

    def pass_on(self, block, j, half):
        for flip in self.multi:
            bit = self.route(flip, half)
            if flip ^ bit == block:
                self.flip_copy(bit, block, j, half).start()
        self.core_copy(block, j, half).start()

    def relay_single(self, j, half):
        for block in self.bits:
            self.flip_copy(block, 0, j, half).wait_recv()
            self.pass_on(block, j, half)

    def relay_multi(self, j, half):
        for block in self.multi:
            bit = self.route(block, half)
            self.flip_copy(bit, block ^ bit, j, half).wait_recv()
            self.pass_on(block, j, half)

    def arrived(self, j):
        for block in range(0, self.n_rows, 2):
            for half in range(2):
                self.core_copy(block, j, half).wait_recv()

    def end(self):
        for half in range(2):
            for k in range(self.n_cols - 1):
                for up in (True, False):
                    pl.when(self.goes_on(up, k))(self.z_copy(up, k, half).wait_send)
            for j in range(self.n_cols + 2):
                for bit in self.bits:
                    self.flip_copy(bit, 0, j, half).wait_send()
                for block in range(0, self.n_rows, 2):
                    self.core_copy(block, j, half).wait_send()
                    if block in self.multi:
                        bit = self.route(block, half)
                        self.flip_copy(bit, block ^ bit, j, half).wait_send()


def fold_kernel(batch, n_rows, n_cols, *refs):
    count_ref, values_in, length_in, third_in, pick_in, owner_in, third_block, second_block = refs[:8]
    out_ref, gram_second_ref, gram_ref, third, second, part_ref, landed = refs[8:15]
    dense, masked, index, fold, values, length, pick_row, owner_row, part_send, part_land, local = refs[15:26]
    gather = Gather(n_rows, n_cols, third, second, gram_second_ref, refs[26:])
    nblk, width = values.shape
    rank, range_rows = second.shape
    third_rows = third.shape[2]
    n_hi = n_cols * third_rows // LO
    part_hi = third_rows // LO
    row, col = gather.row, gather.col
    batches = nblk // batch
    s_piece, g_piece = n_cols, n_cols + 1

    ready = gather.signal()
    sources = [second_block, third_block, values_in, length_in, third_in, pick_in, owner_in]
    targets = [gather.area(0, s_piece), gather.area(0, 0), values, length, index, pick_row, owner_row]
    loads = [pltpu.make_async_copy(a, b, local.at[i]) for i, (a, b) in enumerate(zip(sources, targets))]
    for load in loads:
        load.start()
    ready()
    loads[0].wait()
    for half in range(2):
        gather.own_flips(s_piece, half)
    loads[1].wait()
    for half in range(2):
        gather.own_z(half)
        gather.own_flips(0, half)
    for load in loads[2:]:
        load.wait()

    gram_ref[...] = jnp.zeros_like(gram_ref)
    out_ref[...] = jnp.zeros_like(out_ref)
    lane = lax.broadcasted_iota(jnp.int32, (128, width), 1)
    at_slot = lax.broadcasted_iota(jnp.int32, (128, width), 0)
    for i in range(0, nblk, 128):
        blocks = slice(i, i + 128)
        lengths = jnp.broadcast_to(length[:, blocks], (128, 128)).T
        live = (lane < lengths) & (at_slot + i < count_ref[0])
        masked[blocks, :] = jnp.where(live, values[blocks, :].astype(F32), 0.0)
    given = index[...]
    turned = given
    for j in range(n_cols):
        start = gather.source_of(j) * third_rows
        inside = (given >= start) & (given < start + third_rows)
        turned = jnp.where(inside, given - start + j * third_rows, turned)
    index[...] = turned

    at = lax.broadcasted_iota(jnp.int32, (max(LO, n_hi), width), 0).astype(F32).astype(BF)
    one = jnp.ones((16, width), BF)
    zero = jnp.zeros((16, width), BF)

    def spread(start, first):
        place = index[pl.ds(start, 8), :]
        value = masked[pl.ds(start, 8), :]
        high = lax.shift_right_logical(place, 7).astype(F32)
        low = (place & (LO - 1)).astype(F32)
        for j in range(8):
            high16 = jnp.broadcast_to(high[j : j + 1, :], (16, width)).astype(BF)
            low16 = jnp.broadcast_to(low[j : j + 1, :], (16, width)).astype(BF)
            value16 = jnp.broadcast_to(value[j : j + 1, :], (16, width)).astype(BF)
            left = [jnp.where(at[k : k + 16] == high16, value16, zero) for k in range(0, n_hi, 16)]
            right = [jnp.where(at[k : k + 16] == low16, one, zero) for k in range(0, LO, 16)]
            tile = dot(jnp.concatenate(left, axis=0), jnp.concatenate(right, axis=0), NT)
            dense[pl.ds(first + j, n_hi, stride=batch + 8), :] = tile

    def fold_slot(j, k):
        depth = third_rows // 2
        at_hi = j * part_hi + k * (depth // LO)
        starts = [(at_hi + h) * (batch + 8) for h in range(depth // LO)]
        x = jnp.concatenate([dense[start : start + batch, :] for start in starts], axis=1)
        high = x.astype(BF)
        low = (x - high.astype(F32)).astype(BF)
        piece = third[j, :, k * depth : (k + 1) * depth]
        fold[...] += dot(high, piece, NT) + dot(low, piece, NT)

    def gram_slot(j):
        piece = third[j]
        gram_ref[...] += dot(piece, piece, NT)

    def part_copy(step):
        return pltpu.make_async_remote_copy(
            src_ref=part_ref,
            dst_ref=landed.at[n_cols - step],
            send_sem=part_send.at[step],
            recv_sem=part_land.at[n_cols - step],
            device_id=(row, lax.rem(col + step, n_cols)),
            device_id_type=MESH,
        )

    def part_make():
        gather.arrived(s_piece)
        part_ref[...] = dot(second[gather.rows(0), :], second[...], NT)

    def part_start():
        for step in range(1, n_cols):
            part_copy(step).start()

    def part_sum():
        total = part_ref[...]
        for step in range(1, n_cols):
            part_copy(step).wait_recv()
        for at_col in range(1, n_cols):
            total = total + landed[at_col]
        gram_second_ref[gather.rows(0), :] = total

    def scatter(part):
        columns = slice(part * batch, (part + 1) * batch)
        at_second = lax.broadcasted_iota(jnp.int32, (range_rows, batch), 0) + col * range_rows
        pick = jnp.where(at_second == pick_row[:, columns], 1.0, 0.0).astype(BF)
        contrib = dot(second[...], pick, NN) * fold[...].T
        slab = out_ref.shape[1]
        at_owner = lax.broadcasted_iota(jnp.int32, (slab, batch), 0) + row * slab
        place = jnp.where(at_owner == owner_row[:, columns], 1.0, 0.0).astype(BF)
        high = contrib.astype(BF)
        rest = contrib - high.astype(F32)
        middle = rest.astype(BF)
        low = (rest - middle.astype(F32)).astype(BF)
        out_ref[...] += dot(high, place, NT) + (dot(middle, place, NT) + dot(low, place, NT))

    plan = [(11.3, part_make, ()), (12.3, part_start, ()), (16.0, part_sum, ())]
    due = []
    last = 4.1 * n_cols + 2
    for half in range(2):
        plan.append((4.8 + 0.1 * half, gather.relay_single, (s_piece, half)))
        plan.append((9.6 + 0.1 * half, gather.relay_multi, (s_piece, half)))
        plan.append((last + 0.1 * half, gather.own_flips, (g_piece, half)))
        plan.append((last + 4.0 + 0.3 * half, gather.relay_single, (g_piece, half)))
        plan.append((last + 6.5 + 0.3 * half, gather.relay_multi, (g_piece, half)))
        for j in range(n_cols):
            single = 6.2 + 1.3 * half
            if j > 0:
                plan.append((4.8 + 3.55 * (j - 1) + 1.4 * half, gather.relay_z, (j, half)))
                single = 9.6 + 4.1 * (j - 1) + 2.8 * half
            multi = max(13.7 + 4.6 * j - 0.62 * j * j, 12.1 + 4.1 * (j - 1)) + 1.2 * half
            multi = max(multi, single + 2.5)
            plan.append((single, gather.relay_single, (j, half)))
            plan.append((multi, gather.relay_multi, (j, half)))
            if half:
                due.append(max(multi + 1.6, 19.5 + 1.7 * j))
    plan.sort(key=lambda entry: entry[0])
    steps = batch // CHUNK
    early = {}
    late = []
    for when, act, args in plan:
        step = max(0, int((when - 1.6) / 16.0 * steps))
        if step < steps:
            early.setdefault(step, []).append((act, args))
        else:
            late.append((when, act, args))

    def dispatch(i, low, high):
        if high - low > 1:
            middle = (low + high) // 2
            pl.when(i < middle)(functools.partial(dispatch, i, low, middle))
            pl.when(i >= middle)(functools.partial(dispatch, i, middle, high))
        else:
            for act, args in early.get(low, []):
                act(*args)

    def catch_up(until):
        while late and late[0][0] <= until:
            when, act, args = late.pop(0)
            act(*args)

    for part in range(batches):
        fold[...] = jnp.zeros_like(fold)

        def chunk(i, carry, part=part):
            def eight(k, carry):
                first = pl.multiple_of(i * CHUNK + k * 8, 8)
                spread(pl.multiple_of(part * batch + first, 8), first)
                return carry

            lax.fori_loop(0, CHUNK // 8, eight, 0, unroll=True)
            if part == 0:
                dispatch(i, 0, steps)

            return carry

        lax.fori_loop(0, steps, chunk, 0)
        for j in range(n_cols):
            if part == 0:
                catch_up(due[j])
                gather.arrived(j)
                gram_slot(j)
            for k in range(2):
                fold_slot(j, k)
                if part == 0 and k == 0:
                    catch_up(due[j] + 0.9)
        if part == 0:
            catch_up(due[-1] + 0.5)
        scatter(part)
        catch_up(1000)
    gather.arrived(g_piece)
    for step in range(1, n_cols):
        part_copy(step).wait_send()
    gather.end()


def fold_rows(count, values, length, third, second, owner, third_block, second_block, n_rows, n_cols, slab):
    nblk, width = values.shape
    block, third_rows = third_block.shape
    range_rows = second_block.shape[1]
    rank = block * n_rows
    n_hi = n_cols * third_rows // LO
    batch = nblk
    while n_hi * (batch + 8) * LO * 4 > 20 * 1024 * 1024:
        batch //= 2
    vmem = pl.BlockSpec(memory_space=pltpu.VMEM)
    dma = pltpu.SemaphoreType.DMA
    return pl.pallas_call(
        functools.partial(fold_kernel, batch, n_rows, n_cols),
        in_specs=[pl.BlockSpec(memory_space=pltpu.SMEM)] + [pl.BlockSpec(memory_space=pltpu.HBM)] * 7,
        out_specs=[vmem] * 3,
        out_shape=[jax.ShapeDtypeStruct((rank, slab), F32)] + [jax.ShapeDtypeStruct((rank, rank), F32)] * 2,
        scratch_shapes=[
            pltpu.VMEM((n_cols, rank, third_rows), BF),
            pltpu.VMEM((rank, range_rows), BF),
            pltpu.VMEM((block, rank), F32),
            pltpu.VMEM((n_cols, block, rank), F32),
            pltpu.VMEM((n_hi * (batch + 8), LO), F32),
            pltpu.VMEM((nblk, width), F32),
            pltpu.VMEM((nblk, width), jnp.int32),
            pltpu.VMEM((batch, rank), F32),
            pltpu.VMEM((nblk, width), BF),
            pltpu.VMEM((1, nblk), jnp.int32),
            pltpu.VMEM((1, nblk), jnp.int32),
            pltpu.VMEM((1, nblk), jnp.int32),
            dma((n_cols,)),
            dma((n_cols,)),
            dma((7,)),
            dma((2, n_cols, 2)),
            dma((2, n_cols, 2)),
        ]
        + [dma((n_rows // 2, n_cols + 2, 2))] * 4,
        compiler_params=pltpu.CompilerParams(
            vmem_limit_bytes=58 * 1024 * 1024, collective_id=0, has_side_effects=True
        ),
        name="gather_fold",
    )(count, values, length, third, second, owner, third_block, second_block)


def small_inverse(block):
    n = block.shape[0]
    down = lax.broadcasted_iota(jnp.int32, (n, n), 0)
    across = lax.broadcasted_iota(jnp.int32, (n, n), 1)
    for j in range(n):
        column = block[:, j : j + 1]
        pivot = 1.0 / block[j : j + 1, j : j + 1]
        cleared = jnp.where(across == j, jnp.where(down == j, 1.0, 0.0), block)
        row = cleared[j : j + 1, :] * pivot
        block = jnp.where(down == j, row, cleared - column * row)
    return block


def full_inverse(a, size):
    rank = a.shape[0]
    down = lax.broadcasted_iota(jnp.int32, (rank, size), 0)
    eye = jnp.where(
        lax.broadcasted_iota(jnp.int32, (size, size), 0) == lax.broadcasted_iota(jnp.int32, (size, size), 1), 1.0, 0.0
    )
    for k in range(rank // size):
        s, e = k * size, (k + 1) * size
        inverse = small_inverse(a[s:e, s:e])
        column = jnp.where((down >= s) & (down < e), 0.0, a[:, s:e])
        pieces = [a[s:e, :s]] * (s > 0) + [eye] + [a[s:e, e:]] * (e < rank)
        row = dot(inverse, jnp.concatenate(pieces, axis=1), NN, EXACT)
        zero = jnp.zeros((rank, size), F32)
        pieces = [a[:, :s]] * (s > 0) + [zero] + [a[:, e:]] * (e < rank)
        a = jnp.concatenate(pieces, axis=1) - dot(column, row, NN, EXACT)
        pieces = [a[:s]] * (s > 0) + [row] + [a[e:]] * (e < rank)
        a = jnp.concatenate(pieces, axis=0)
    return a


def reach(x):
    return jnp.max(jnp.sum(jnp.abs(x), axis=1, keepdims=True))


def solve_kernel(size, scale, left_ref, right_ref, rows_ref, out_ref, power):
    rank = left_ref.shape[1]
    a = (left_ref[...] / scale[0]) * (right_ref[...] / scale[1])
    down = lax.broadcasted_iota(jnp.int32, (rank, rank), 0)
    across = lax.broadcasted_iota(jnp.int32, (rank, rank), 1)
    diagonal = jnp.where(down == across, a, 0.0)
    down_scale = lax.rsqrt(jnp.sum(diagonal, axis=1, keepdims=True))
    across_scale = lax.rsqrt(jnp.sum(diagonal, axis=0, keepdims=True))
    off = (a * down_scale) * across_scale - jnp.where(down == across, 1.0, 0.0)
    near = reach(off) < 0.5

    @pl.when(near)
    def _():
        square = dot(off, off, NN, EXACT)
        rows = rows_ref[...] * down_scale
        rows = rows - dot(off, rows, NN, EXACT)
        rows = rows + dot(square, rows, NN, EXACT)
        out_ref[...] = rows * down_scale
        power[...] = square

        def more(left):
            return left * left > 1e-9

        def factor(left):
            square = dot(power[...], power[...], NN, EXACT)
            power[...] = square
            rows = out_ref[...] / down_scale
            out_ref[...] = (rows + dot(square, rows, NN, EXACT)) * down_scale
            return reach(square)

        lax.while_loop(more, factor, reach(square))

    @pl.when(jnp.logical_not(near))
    def _():
        out_ref[...] = dot(full_inverse(a, size), rows_ref[...], NN, EXACT)


def solve(left, right, rows, scale):
    return pl.pallas_call(
        functools.partial(solve_kernel, 32, scale),
        out_shape=jax.ShapeDtypeStruct(rows.shape, F32),
        in_specs=[pl.BlockSpec(memory_space=pltpu.VMEM)] * 3,
        out_specs=pl.BlockSpec(memory_space=pltpu.VMEM),
        scratch_shapes=[pltpu.VMEM(left.shape, F32)],
        name="solve",
    )(left, right, rows)


def exchange_kernel(n_rows, n_cols, tiles_in, out_ref, tiles_ref, middle, landed, own, send_a, land_a, send_b, land_b):
    row, col = lax.axis_index("rows"), lax.axis_index("cols")
    share = n_rows // n_cols
    block = tiles_ref.shape[0] // n_rows
    load = pltpu.make_async_copy(tiles_in, tiles_ref, own)
    load.start()
    slab = tiles_ref.shape[1]
    barrier = pltpu.get_barrier_semaphore()
    near = [(flipped(row, f), col) for f in range(1, n_rows)]
    near += [(row, lax.rem(col + d, n_cols)) for d in range(1, n_cols)]
    for target in near:
        pl.semaphore_signal(barrier, inc=1, device_id=target, device_id_type=MESH)
    pl.semaphore_wait(barrier, len(near))
    load.wait()

    def tile(flip):
        start = pl.multiple_of(flipped(row, flip) * block, block)
        return tiles_ref.at[pl.ds(start, block), :]

    def across(flip):
        return pltpu.make_async_remote_copy(
            src_ref=tile(flip),
            dst_ref=middle.at[flip],
            send_sem=send_a.at[flip],
            recv_sem=land_a.at[flip],
            device_id=(flipped(row, flip), col),
            device_id_type=MESH,
        )

    def along(flip):
        source = flipped(row, flip)
        home = source // share
        return home, lax.rem(source, share), pltpu.make_async_remote_copy(
            src_ref=middle.at[flip] if flip else tile(0),
            dst_ref=landed.at[lax.rem(source, share) * n_cols + col],
            send_sem=send_b.at[flip],
            recv_sem=land_b.at[lax.rem(source, share) * n_cols + col],
            device_id=(row, home),
            device_id_type=MESH,
        )

    far = list(range(n_rows // 2, n_rows))
    order = list(range(1, n_rows // 2))
    for flip in far[::-1] + order[::-1]:
        across(flip).start()
    for flip in [0] + [f for f in order if f == 1] + far + [f for f in order if f > 1]:
        if flip:
            across(flip).wait_recv()
        home, at, copy = along(flip)
        pl.when(home != col)(copy.start)

        @pl.when(home == col)
        def _():
            landed[at * n_cols + col] = middle[flip] if flip else tile(0)[...]

    def arrive(at, step):
        source = lax.rem(col + step, n_cols)
        return source, pltpu.make_async_remote_copy(
            src_ref=middle.at[0],
            dst_ref=landed.at[at * n_cols + source],
            send_sem=send_b.at[0],
            recv_sem=land_b.at[at * n_cols + source],
            device_id=(row, source),
            device_id_type=MESH,
        )

    for at in range(share):
        for step in range(1, n_cols):
            arrive(at, step)[1].wait_recv()
        total = landed[at * n_cols]
        for c in range(1, n_cols):
            total = total + landed[at * n_cols + c]
        out_ref[:, at * slab : (at + 1) * slab] = total
    for flip in range(n_rows):
        if flip:
            across(flip).wait_send()
        home, at, copy = along(flip)
        pl.when(home != col)(copy.wait_send)


def exchange(tiles, n_rows, n_cols):
    rank, slab = tiles.shape
    block = rank // n_rows
    dma = pltpu.SemaphoreType.DMA
    return pl.pallas_call(
        functools.partial(exchange_kernel, n_rows, n_cols),
        in_specs=[pl.BlockSpec(memory_space=pltpu.HBM)],
        out_specs=pl.BlockSpec(memory_space=pltpu.VMEM),
        out_shape=jax.ShapeDtypeStruct((block, n_rows // n_cols * slab), F32),
        scratch_shapes=[pltpu.VMEM((rank, slab), F32)]
        + [pltpu.VMEM((n_rows, block, slab), F32)] * 2
        + [dma]
        + [dma((n_rows,))] * 4,
        compiler_params=pltpu.CompilerParams(
            vmem_limit_bytes=58 * 1024 * 1024, collective_id=1, has_side_effects=True
        ),
        name="exchange",
    )(tiles)


def per_device(
    block_values,
    block_length,
    block_owner,
    block_second,
    block_third,
    live_blocks,
    second_factor,
    third_factor,
):
    n_rows = lax.axis_size("rows")
    n_cols = lax.axis_size("cols")
    nblk = block_values.shape[0]
    range_rows = second_factor.shape[0]
    third_rows = third_factor.shape[0]
    slab = range_rows * n_cols // n_rows
    rows, gram_second, gram_third = fold_rows(
        live_blocks,
        block_values,
        block_length.reshape(1, nblk),
        block_third,
        block_second.reshape(1, nblk),
        block_owner.reshape(1, nblk),
        third_factor.T,
        second_factor.T,
        n_rows,
        n_cols,
        slab,
    )
    solved = solve(gram_second, gram_third, rows, (range_rows * n_cols, third_rows * n_cols))
    return exchange(solved, n_rows, n_cols).T


def solution(mesh):
    return jax.shard_map(
        per_device,
        mesh=mesh,
        in_specs=(
            P(("rows", "cols"), None),
            P(("rows", "cols")),
            P(("rows", "cols")),
            P(("rows", "cols")),
            P(("rows", "cols"), None),
            P(("rows", "cols")),
            P("cols", "rows"),
            P("cols", "rows"),
        ),
        out_specs=P("cols", "rows"),
        check_vma=False,
    )
```

```python
import functools

import jax
import jax.numpy as jnp
from jax import lax
from jax.experimental import pallas as pl
from jax.experimental.pallas import tpu as pltpu
from jax.sharding import PartitionSpec as P

LO = 128
CHUNK = 32
BF = jnp.bfloat16
F32 = jnp.float32
NT = (((1,), (1,)), ((), ()))
NN = (((1,), (0,)), ((), ()))
EXACT = lax.Precision.HIGHEST
MESH = pl.DeviceIdType.MESH


def dot(a, b, dims, precision=None):
    return lax.dot_general(a, b, dims, precision=precision, preferred_element_type=F32)


def flipped(row, flip):
    target = row
    bit = 1
    while bit <= flip:
        if flip & bit:
            target = target + bit - 2 * bit * lax.rem(row // bit, 2)
        bit *= 2
    return target


class Gather:
    def __init__(self, n_rows, n_cols, third, second, gram, sems):
        self.n_rows, self.n_cols = n_rows, n_cols
        self.third, self.second, self.gram = third, second, gram
        self.send_z, self.land_z, self.send_f, self.land_f, self.hand, self.take = sems
        self.rank = second.shape[0] // n_rows
        self.row, self.col = lax.axis_index("rows"), lax.axis_index("cols")
        self.partner = flipped(self.row, 1)
        self.bits = [b for b in (2**i for i in range(1, 16)) if b < n_rows]
        self.multi = [f for f in range(2, n_rows, 2) if f not in self.bits]
        self.near = []
        for c in range(n_cols):
            self.near.append(sorted(range(n_cols), key=lambda a: (abs(a - c), a)))

    def by_col(self, table):
        return sum((self.col == c).astype(jnp.int32) * table[c] for c in range(self.n_cols))

    def position(self, up, k, there=0):
        table = []
        for c in range(self.n_cols):
            source = c - k if up else c + k
            holder = c + there
            known = 0 <= source < self.n_cols and 0 <= holder < self.n_cols
            table.append(self.near[holder].index(source) if known else 0)
        return self.by_col(table)

    def source_of(self, j):
        return self.by_col([self.near[c][j] for c in range(self.n_cols)])

    def rows(self, block, half=None):
        start = flipped(self.row, block) * self.rank
        size = self.rank
        if half is not None:
            size = self.rank // 2
            start = start + half * size
        return pl.ds(pl.multiple_of(start, size), size)

    def area(self, block, j, half=None):
        if isinstance(j, int) and j == self.n_cols:
            return self.second.at[self.rows(block, half), :]
        if isinstance(j, int) and j == self.n_cols + 1:
            return self.gram.at[self.rows(block, half), :]
        return self.third.at[j, self.rows(block, half), :]

    def z_copy(self, up, k, half):
        step = 1 if up else -1
        return pltpu.make_async_remote_copy(
            src_ref=self.area(0, self.position(up, k), half),
            dst_ref=self.area(0, self.position(up, k, step), half),
            send_sem=self.send_z.at[int(up), k, half],
            recv_sem=self.land_z.at[int(up), k, half],
            device_id=(self.row, lax.rem(self.col + step + self.n_cols, self.n_cols)),
            device_id_type=MESH,
        )

    def goes_on(self, up, k):
        return (self.col >= k) & (self.col + 1 < self.n_cols) if up else (self.col + k < self.n_cols) & (self.col >= 1)

    def relay_z(self, k, half):
        for up in (True, False):
            here = self.col >= k if up else self.col + k < self.n_cols

            @pl.when(here)
            def _():
                self.z_copy(up, k - 1, half).wait_recv()

            pl.when(self.goes_on(up, k))(self.z_copy(up, k, half).start)

            @pl.when(here)
            def _():
                self.own_flips(self.position(up, k), half)

    def flip_copy(self, bit, block, j, half):
        there = block ^ bit
        return pltpu.make_async_remote_copy(
            src_ref=self.area(block, j, half),
            dst_ref=self.area(block, j, half),
            send_sem=self.send_f.at[there // 2, j, half],
            recv_sem=self.land_f.at[there // 2, j, half],
            device_id=(flipped(self.row, bit), self.col),
            device_id_type=MESH,
        )

    def route(self, flip, half):
        bits = [b for b in self.bits if flip & b]
        return bits[0] if half == 0 else bits[-1]

    def core_copy(self, block, j, half):
        return pltpu.make_async_remote_copy(
            src_ref=self.area(block, j, half),
            dst_ref=self.area(block, j, half),
            send_sem=self.hand.at[block // 2, j, half],
            recv_sem=self.take.at[block // 2, j, half],
            device_id=(self.partner, self.col),
            device_id_type=MESH,
        )

    def signal(self):
        barrier = pltpu.get_barrier_semaphore()
        near = [(self.partner, self.col)]
        near += [(self.row, lax.rem(self.col + d, self.n_cols)) for d in range(1, self.n_cols)]
        near += [(flipped(self.row, f), self.col) for f in range(2, self.n_rows, 2)]
        for target in near:
            pl.semaphore_signal(barrier, inc=1, device_id=target, device_id_type=MESH)
        return functools.partial(pl.semaphore_wait, barrier, len(near))

    def own_z(self, half):
        for up in (True, False):
            pl.when(self.goes_on(up, 0))(self.z_copy(up, 0, half).start)

    def own_flips(self, j, half):
        for bit in self.bits:
            self.flip_copy(bit, 0, j, half).start()
        self.core_copy(0, j, half).start()

    def pass_on(self, block, j, half):
        for flip in self.multi:
            bit = self.route(flip, half)
            if flip ^ bit == block:
                self.flip_copy(bit, block, j, half).start()
        self.core_copy(block, j, half).start()

    def relay_single(self, j, half):
        for block in self.bits:
            self.flip_copy(block, 0, j, half).wait_recv()
            self.pass_on(block, j, half)

    def relay_multi(self, j, half):
        for block in self.multi:
            bit = self.route(block, half)
            self.flip_copy(bit, block ^ bit, j, half).wait_recv()
            self.pass_on(block, j, half)

    def arrived(self, j):
        for block in range(0, self.n_rows, 2):
            for half in range(2):
                self.core_copy(block, j, half).wait_recv()

    def end(self):
        for half in range(2):
            for k in range(self.n_cols - 1):
                for up in (True, False):
                    pl.when(self.goes_on(up, k))(self.z_copy(up, k, half).wait_send)
            for j in range(self.n_cols + 2):
                for bit in self.bits:
                    self.flip_copy(bit, 0, j, half).wait_send()
                for block in range(0, self.n_rows, 2):
                    self.core_copy(block, j, half).wait_send()
                    if block in self.multi:
                        bit = self.route(block, half)
                        self.flip_copy(bit, block ^ bit, j, half).wait_send()


def fold_kernel(batch, n_rows, n_cols, *refs):
    count_ref, values_in, length_in, third_in, pick_in, owner_in, third_block, second_block = refs[:8]
    out_ref, gram_second_ref, gram_ref, third, second, part_ref, landed = refs[8:15]
    dense, masked, index, fold, values, length, pick_row, owner_row, part_send, part_land, local = refs[15:26]
    gather = Gather(n_rows, n_cols, third, second, gram_second_ref, refs[26:])
    nblk, width = values.shape
    rank, range_rows = second.shape
    third_rows = third.shape[2]
    n_hi = n_cols * third_rows // LO
    part_hi = third_rows // LO
    row, col = gather.row, gather.col
    batches = nblk // batch
    s_piece, g_piece = n_cols, n_cols + 1

    ready = gather.signal()
    sources = [second_block, third_block, values_in, length_in, third_in, pick_in, owner_in]
    targets = [gather.area(0, s_piece), gather.area(0, 0), values, length, index, pick_row, owner_row]
    loads = [pltpu.make_async_copy(a, b, local.at[i]) for i, (a, b) in enumerate(zip(sources, targets))]
    for load in loads:
        load.start()
    ready()
    loads[0].wait()
    for half in range(2):
        gather.own_flips(s_piece, half)
    loads[1].wait()
    for half in range(2):
        gather.own_z(half)
        gather.own_flips(0, half)
    for load in loads[2:]:
        load.wait()

    gram_ref[...] = jnp.zeros_like(gram_ref)
    out_ref[...] = jnp.zeros_like(out_ref)
    lane = lax.broadcasted_iota(jnp.int32, (128, width), 1)
    at_slot = lax.broadcasted_iota(jnp.int32, (128, width), 0)
    for i in range(0, nblk, 128):
        blocks = slice(i, i + 128)
        lengths = jnp.broadcast_to(length[:, blocks], (128, 128)).T
        live = (lane < lengths) & (at_slot + i < count_ref[0])
        masked[blocks, :] = jnp.where(live, values[blocks, :].astype(F32), 0.0)
    given = index[...]
    turned = given
    for j in range(n_cols):
        start = gather.source_of(j) * third_rows
        inside = (given >= start) & (given < start + third_rows)
        turned = jnp.where(inside, given - start + j * third_rows, turned)
    index[...] = turned

    at = lax.broadcasted_iota(jnp.int32, (max(LO, n_hi), width), 0).astype(F32).astype(BF)
    one = jnp.ones((16, width), BF)
    zero = jnp.zeros((16, width), BF)

    def spread(start, first):
        place = index[pl.ds(start, 8), :]
        value = masked[pl.ds(start, 8), :]
        high = lax.shift_right_logical(place, 7).astype(F32)
        low = (place & (LO - 1)).astype(F32)
        for j in range(8):
            high16 = jnp.broadcast_to(high[j : j + 1, :], (16, width)).astype(BF)
            low16 = jnp.broadcast_to(low[j : j + 1, :], (16, width)).astype(BF)
            value16 = jnp.broadcast_to(value[j : j + 1, :], (16, width)).astype(BF)
            left = [jnp.where(at[k : k + 16] == high16, value16, zero) for k in range(0, n_hi, 16)]
            right = [jnp.where(at[k : k + 16] == low16, one, zero) for k in range(0, LO, 16)]
            tile = dot(jnp.concatenate(left, axis=0), jnp.concatenate(right, axis=0), NT)
            dense[pl.ds(first + j, n_hi, stride=batch + 8), :] = tile

    def fold_slot(j, k):
        depth = third_rows // 2
        at_hi = j * part_hi + k * (depth // LO)
        starts = [(at_hi + h) * (batch + 8) for h in range(depth // LO)]
        x = jnp.concatenate([dense[start : start + batch, :] for start in starts], axis=1)
        high = x.astype(BF)
        low = (x - high.astype(F32)).astype(BF)
        piece = third[j, :, k * depth : (k + 1) * depth]
        fold[...] += dot(high, piece, NT) + dot(low, piece, NT)

    def gram_slot(j):
        piece = third[j]
        gram_ref[...] += dot(piece, piece, NT)

    def part_copy(step):
        return pltpu.make_async_remote_copy(
            src_ref=part_ref,
            dst_ref=landed.at[n_cols - step],
            send_sem=part_send.at[step],
            recv_sem=part_land.at[n_cols - step],
            device_id=(row, lax.rem(col + step, n_cols)),
            device_id_type=MESH,
        )

    def part_make():
        gather.arrived(s_piece)
        part_ref[...] = dot(second[gather.rows(0), :], second[...], NT)

    def part_start():
        for step in range(1, n_cols):
            part_copy(step).start()

    def part_sum():
        total = part_ref[...]
        for step in range(1, n_cols):
            part_copy(step).wait_recv()
        for at_col in range(1, n_cols):
            total = total + landed[at_col]
        gram_second_ref[gather.rows(0), :] = total

    def scatter(part):
        columns = slice(part * batch, (part + 1) * batch)
        at_second = lax.broadcasted_iota(jnp.int32, (range_rows, batch), 0) + col * range_rows
        pick = jnp.where(at_second == pick_row[:, columns], 1.0, 0.0).astype(BF)
        contrib = dot(second[...], pick, NN) * fold[...].T
        slab = out_ref.shape[1]
        at_owner = lax.broadcasted_iota(jnp.int32, (slab, batch), 0) + row * slab
        place = jnp.where(at_owner == owner_row[:, columns], 1.0, 0.0).astype(BF)
        high = contrib.astype(BF)
        rest = contrib - high.astype(F32)
        middle = rest.astype(BF)
        low = (rest - middle.astype(F32)).astype(BF)
        out_ref[...] += dot(high, place, NT) + (dot(middle, place, NT) + dot(low, place, NT))

    plan = [(11.3, part_make, ()), (12.3, part_start, ()), (16.0, part_sum, ())]
    due = []
    last = 4.1 * n_cols + 2
    for half in range(2):
        plan.append((4.8 + 0.1 * half, gather.relay_single, (s_piece, half)))
        plan.append((9.6 + 0.1 * half, gather.relay_multi, (s_piece, half)))
        plan.append((last + 0.1 * half, gather.own_flips, (g_piece, half)))
        plan.append((last + 4.0 + 0.3 * half, gather.relay_single, (g_piece, half)))
        plan.append((last + 6.5 + 0.3 * half, gather.relay_multi, (g_piece, half)))
        for j in range(n_cols):
            single = 6.2 + 1.3 * half
            if j > 0:
                plan.append((4.8 + 3.55 * (j - 1) + 1.4 * half, gather.relay_z, (j, half)))
                single = 9.6 + 4.1 * (j - 1) + 2.8 * half
            multi = max(13.7 + 4.6 * j - 0.62 * j * j, 12.1 + 4.1 * (j - 1)) + 1.2 * half
            multi = max(multi, single + 2.5)
            plan.append((single, gather.relay_single, (j, half)))
            plan.append((multi, gather.relay_multi, (j, half)))
            if half:
                due.append(max(multi + 1.6, 20.2 + 1.7 * j))
    plan.sort(key=lambda entry: entry[0])
    steps = batch // CHUNK
    early = {}
    late = []
    for when, act, args in plan:
        step = max(0, int((when - 1.6) / 16.0 * steps))
        if step < steps:
            early.setdefault(step, []).append((act, args))
        else:
            late.append((when, act, args))

    def dispatch(i, low, high):
        if high - low > 1:
            middle = (low + high) // 2
            pl.when(i < middle)(functools.partial(dispatch, i, low, middle))
            pl.when(i >= middle)(functools.partial(dispatch, i, middle, high))
        else:
            for act, args in early.get(low, []):
                act(*args)

    def catch_up(until):
        while late and late[0][0] <= until:
            when, act, args = late.pop(0)
            act(*args)

    for part in range(batches):
        fold[...] = jnp.zeros_like(fold)

        def chunk(i, carry, part=part):
            def eight(k, carry):
                first = pl.multiple_of(i * CHUNK + k * 8, 8)
                spread(pl.multiple_of(part * batch + first, 8), first)
                return carry

            lax.fori_loop(0, CHUNK // 8, eight, 0, unroll=True)
            if part == 0:
                dispatch(i, 0, steps)

            return carry

        lax.fori_loop(0, steps, chunk, 0)
        for j in range(n_cols):
            if part == 0:
                catch_up(due[j])
                gather.arrived(j)
                gram_slot(j)
            for k in range(2):
                fold_slot(j, k)
                if part == 0 and k == 0:
                    catch_up(due[j] + 0.9)
        if part == 0:
            catch_up(due[-1] + 0.5)
        scatter(part)
        catch_up(1000)
    gather.arrived(g_piece)
    for step in range(1, n_cols):
        part_copy(step).wait_send()
    gather.end()


def fold_rows(count, values, length, third, second, owner, third_block, second_block, n_rows, n_cols, slab):
    nblk, width = values.shape
    block, third_rows = third_block.shape
    range_rows = second_block.shape[1]
    rank = block * n_rows
    n_hi = n_cols * third_rows // LO
    batch = nblk
    while n_hi * (batch + 8) * LO * 4 > 20 * 1024 * 1024:
        batch //= 2
    vmem = pl.BlockSpec(memory_space=pltpu.VMEM)
    dma = pltpu.SemaphoreType.DMA
    return pl.pallas_call(
        functools.partial(fold_kernel, batch, n_rows, n_cols),
        in_specs=[pl.BlockSpec(memory_space=pltpu.SMEM)] + [pl.BlockSpec(memory_space=pltpu.HBM)] * 7,
        out_specs=[vmem] * 3,
        out_shape=[jax.ShapeDtypeStruct((rank, slab), F32)] + [jax.ShapeDtypeStruct((rank, rank), F32)] * 2,
        scratch_shapes=[
            pltpu.VMEM((n_cols, rank, third_rows), BF),
            pltpu.VMEM((rank, range_rows), BF),
            pltpu.VMEM((block, rank), F32),
            pltpu.VMEM((n_cols, block, rank), F32),
            pltpu.VMEM((n_hi * (batch + 8), LO), F32),
            pltpu.VMEM((nblk, width), F32),
            pltpu.VMEM((nblk, width), jnp.int32),
            pltpu.VMEM((batch, rank), F32),
            pltpu.VMEM((nblk, width), BF),
            pltpu.VMEM((1, nblk), jnp.int32),
            pltpu.VMEM((1, nblk), jnp.int32),
            pltpu.VMEM((1, nblk), jnp.int32),
            dma((n_cols,)),
            dma((n_cols,)),
            dma((7,)),
            dma((2, n_cols, 2)),
            dma((2, n_cols, 2)),
        ]
        + [dma((n_rows // 2, n_cols + 2, 2))] * 4,
        compiler_params=pltpu.CompilerParams(
            vmem_limit_bytes=58 * 1024 * 1024, collective_id=0, has_side_effects=True
        ),
        name="gather_fold",
    )(count, values, length, third, second, owner, third_block, second_block)


def small_inverse(block):
    n = block.shape[0]
    down = lax.broadcasted_iota(jnp.int32, (n, n), 0)
    across = lax.broadcasted_iota(jnp.int32, (n, n), 1)
    for j in range(n):
        column = block[:, j : j + 1]
        pivot = 1.0 / block[j : j + 1, j : j + 1]
        cleared = jnp.where(across == j, jnp.where(down == j, 1.0, 0.0), block)
        row = cleared[j : j + 1, :] * pivot
        block = jnp.where(down == j, row, cleared - column * row)
    return block


def full_inverse(a, size):
    rank = a.shape[0]
    down = lax.broadcasted_iota(jnp.int32, (rank, size), 0)
    eye = jnp.where(
        lax.broadcasted_iota(jnp.int32, (size, size), 0) == lax.broadcasted_iota(jnp.int32, (size, size), 1), 1.0, 0.0
    )
    for k in range(rank // size):
        s, e = k * size, (k + 1) * size
        inverse = small_inverse(a[s:e, s:e])
        column = jnp.where((down >= s) & (down < e), 0.0, a[:, s:e])
        pieces = [a[s:e, :s]] * (s > 0) + [eye] + [a[s:e, e:]] * (e < rank)
        row = dot(inverse, jnp.concatenate(pieces, axis=1), NN, EXACT)
        zero = jnp.zeros((rank, size), F32)
        pieces = [a[:, :s]] * (s > 0) + [zero] + [a[:, e:]] * (e < rank)
        a = jnp.concatenate(pieces, axis=1) - dot(column, row, NN, EXACT)
        pieces = [a[:s]] * (s > 0) + [row] + [a[e:]] * (e < rank)
        a = jnp.concatenate(pieces, axis=0)
    return a


def reach(x):
    return jnp.max(jnp.sum(jnp.abs(x), axis=1, keepdims=True))


def solve_kernel(size, scale, left_ref, right_ref, rows_ref, out_ref, power):
    rank = left_ref.shape[1]
    a = (left_ref[...] / scale[0]) * (right_ref[...] / scale[1])
    down = lax.broadcasted_iota(jnp.int32, (rank, rank), 0)
    across = lax.broadcasted_iota(jnp.int32, (rank, rank), 1)
    diagonal = jnp.where(down == across, a, 0.0)
    down_scale = lax.rsqrt(jnp.sum(diagonal, axis=1, keepdims=True))
    across_scale = lax.rsqrt(jnp.sum(diagonal, axis=0, keepdims=True))
    off = (a * down_scale) * across_scale - jnp.where(down == across, 1.0, 0.0)
    near = reach(off) < 0.5

    @pl.when(near)
    def _():
        square = dot(off, off, NN, EXACT)
        rows = rows_ref[...] * down_scale
        rows = rows - dot(off, rows, NN, EXACT)
        rows = rows + dot(square, rows, NN, EXACT)
        out_ref[...] = rows * down_scale
        power[...] = square

        def more(left):
            return left * left > 1e-9

        def factor(left):
            square = dot(power[...], power[...], NN, EXACT)
            power[...] = square
            rows = out_ref[...] / down_scale
            out_ref[...] = (rows + dot(square, rows, NN, EXACT)) * down_scale
            return reach(square)

        lax.while_loop(more, factor, reach(square))

    @pl.when(jnp.logical_not(near))
    def _():
        out_ref[...] = dot(full_inverse(a, size), rows_ref[...], NN, EXACT)


def solve(left, right, rows, scale):
    return pl.pallas_call(
        functools.partial(solve_kernel, 32, scale),
        out_shape=jax.ShapeDtypeStruct(rows.shape, F32),
        in_specs=[pl.BlockSpec(memory_space=pltpu.VMEM)] * 3,
        out_specs=pl.BlockSpec(memory_space=pltpu.VMEM),
        scratch_shapes=[pltpu.VMEM(left.shape, F32)],
        name="solve",
    )(left, right, rows)


def exchange_kernel(n_rows, n_cols, tiles_in, out_ref, tiles_ref, middle, landed, own, send_a, land_a, send_b, land_b):
    row, col = lax.axis_index("rows"), lax.axis_index("cols")
    share = n_rows // n_cols
    block = tiles_ref.shape[0] // n_rows
    load = pltpu.make_async_copy(tiles_in, tiles_ref, own)
    load.start()
    slab = tiles_ref.shape[1]
    barrier = pltpu.get_barrier_semaphore()
    near = [(flipped(row, f), col) for f in range(1, n_rows)]
    near += [(row, lax.rem(col + d, n_cols)) for d in range(1, n_cols)]
    for target in near:
        pl.semaphore_signal(barrier, inc=1, device_id=target, device_id_type=MESH)
    pl.semaphore_wait(barrier, len(near))
    load.wait()

    def tile(flip):
        start = pl.multiple_of(flipped(row, flip) * block, block)
        return tiles_ref.at[pl.ds(start, block), :]

    def across(flip):
        return pltpu.make_async_remote_copy(
            src_ref=tile(flip),
            dst_ref=middle.at[flip],
            send_sem=send_a.at[flip],
            recv_sem=land_a.at[flip],
            device_id=(flipped(row, flip), col),
            device_id_type=MESH,
        )

    def along(flip):
        source = flipped(row, flip)
        home = source // share
        return home, lax.rem(source, share), pltpu.make_async_remote_copy(
            src_ref=middle.at[flip] if flip else tile(0),
            dst_ref=landed.at[lax.rem(source, share) * n_cols + col],
            send_sem=send_b.at[flip],
            recv_sem=land_b.at[lax.rem(source, share) * n_cols + col],
            device_id=(row, home),
            device_id_type=MESH,
        )

    far = list(range(n_rows // 2, n_rows))
    order = list(range(1, n_rows // 2))
    for flip in order[::-1] + far[::-1]:
        across(flip).start()
    for flip in [0] + order + far:
        if flip:
            across(flip).wait_recv()
        home, at, copy = along(flip)
        pl.when(home != col)(copy.start)

        @pl.when(home == col)
        def _():
            landed[at * n_cols + col] = middle[flip] if flip else tile(0)[...]

    def arrive(at, step):
        source = lax.rem(col + step, n_cols)
        return source, pltpu.make_async_remote_copy(
            src_ref=middle.at[0],
            dst_ref=landed.at[at * n_cols + source],
            send_sem=send_b.at[0],
            recv_sem=land_b.at[at * n_cols + source],
            device_id=(row, source),
            device_id_type=MESH,
        )

    for at in range(share):
        for step in range(1, n_cols):
            arrive(at, step)[1].wait_recv()
        total = landed[at * n_cols]
        for c in range(1, n_cols):
            total = total + landed[at * n_cols + c]
        out_ref[:, at * slab : (at + 1) * slab] = total
    for flip in range(n_rows):
        if flip:
            across(flip).wait_send()
        home, at, copy = along(flip)
        pl.when(home != col)(copy.wait_send)


def exchange(tiles, n_rows, n_cols):
    rank, slab = tiles.shape
    block = rank // n_rows
    dma = pltpu.SemaphoreType.DMA
    return pl.pallas_call(
        functools.partial(exchange_kernel, n_rows, n_cols),
        in_specs=[pl.BlockSpec(memory_space=pltpu.HBM)],
        out_specs=pl.BlockSpec(memory_space=pltpu.VMEM),
        out_shape=jax.ShapeDtypeStruct((block, n_rows // n_cols * slab), F32),
        scratch_shapes=[pltpu.VMEM((rank, slab), F32)]
        + [pltpu.VMEM((n_rows, block, slab), F32)] * 2
        + [dma]
        + [dma((n_rows,))] * 4,
        compiler_params=pltpu.CompilerParams(
            vmem_limit_bytes=58 * 1024 * 1024, collective_id=1, has_side_effects=True
        ),
        name="exchange",
    )(tiles)


def per_device(
    block_values,
    block_length,
    block_owner,
    block_second,
    block_third,
    live_blocks,
    second_factor,
    third_factor,
):
    n_rows = lax.axis_size("rows")
    n_cols = lax.axis_size("cols")
    nblk = block_values.shape[0]
    range_rows = second_factor.shape[0]
    third_rows = third_factor.shape[0]
    slab = range_rows * n_cols // n_rows
    rows, gram_second, gram_third = fold_rows(
        live_blocks,
        block_values,
        block_length.reshape(1, nblk),
        block_third,
        block_second.reshape(1, nblk),
        block_owner.reshape(1, nblk),
        third_factor.T,
        second_factor.T,
        n_rows,
        n_cols,
        slab,
    )
    solved = solve(gram_second, gram_third, rows, (range_rows * n_cols, third_rows * n_cols))
    return exchange(solved, n_rows, n_cols).T


def solution(mesh):
    return jax.shard_map(
        per_device,
        mesh=mesh,
        in_specs=(
            P(("rows", "cols"), None),
            P(("rows", "cols")),
            P(("rows", "cols")),
            P(("rows", "cols")),
            P(("rows", "cols"), None),
            P(("rows", "cols")),
            P("cols", "rows"),
            P("cols", "rows"),
        ),
        out_specs=P("cols", "rows"),
        check_vma=False,
    )
```
